32 devices in a mesh: batch: 2 (over x), items: 16 (over z, y, core).
Axes of the slice: x: 2, y: 2, z: 4, core: 2. Of those that a mesh axis runs over, the one named last changes fastest.
Arguments:
- users: bfloat16 [1280, 256], P(('batch', 'items')), may hold values from -6 to 6
- items: bfloat16 [8192, 256], P(('batch', 'items')), may hold values from -6 to 6
- pos_ids: int32 [1280], P(('batch', 'items')), may hold values from 0 to 8191
Outputs:
- loss: float32 [1280], P(('batch', 'items'))
- user_grad: float32 [1280, 256], P(('batch', 'items'))
- item_grad: float32 [8192, 256], P(('batch', 'items'))
The draws below stay inside these ranges and needn't reach their ends.
All inputs are finite; a program needn't handle non-finite values.
Results may differ from the reference program's by a relative error of at most 0.0015.
Values may be sent and summed in bfloat16 or wider, within the bound.
A program may use at most 64 MiB of HBM per device.

```python
import math
import jax
import jax.numpy as jnp
from jax import lax

E = 256
USERS = 1280
ITEMS = 8192


def joint_towers(key):
    base = jax.random.fold_in(key, 7)
    key_user, key_item, key_pick, key_flag, key_sign, key_align, key_perm = jax.random.split(base, 7)
    users = jnp.clip(jax.random.normal(key_user, (USERS, E), jnp.float32), -6.0, 6.0)
    bank = jnp.clip(0.125 * jax.random.normal(key_item, (ITEMS, E), jnp.float32), -0.75, 0.75)
    user_level = 5.0
    item_level = 320.0 / (user_level * E)
    signs = (2 * jax.random.randint(key_sign, (USERS, E), 0, 2) - 1).astype(jnp.float32)
    aligned = jax.random.randint(key_align, (USERS,), 0, 16) == 0
    users = jnp.where(aligned[:, None], user_level * signs, users)
    users = users.astype(jnp.bfloat16).astype(jnp.float32)
    order = jax.random.permutation(key_perm, ITEMS).astype(jnp.int32)
    rank = jnp.argsort(order).astype(jnp.int32)
    owned = rank < USERS
    partner = jnp.minimum(rank, USERS - 1)
    match = owned & aligned[partner]
    bank = jnp.where(match[:, None], item_level * signs[partner], bank)
    return (users, bank)


def draw_users(key, part):
    return joint_towers(key)[0].astype(jnp.bfloat16)


def draw_items(key, part):
    return joint_towers(key)[1].astype(jnp.bfloat16)


def place_ends(drawn, stream_key, least, high):
    dims = drawn.shape
    index_at = [jax.random.randint(jax.random.fold_in(stream_key, axis), (), 0, dims[axis]) for axis in range(len(dims))]
    drawn = drawn.at[tuple(index_at)].set(least)
    longest = dims.index(max(dims))
    index_at[longest] = (index_at[longest] + 1) % dims[longest]
    return drawn.at[tuple(index_at)].set(high)


def setup_inputs(seed: int = 0) -> dict:
    keys = jax.random.split(jax.random.key(seed), 4)
    return {
        "users": draw_users(jax.random.fold_in(keys[3], 71), 0),
        "items": draw_items(jax.random.fold_in(keys[3], 71), 0),
        "pos_ids": place_ends(jax.random.randint(keys[2], (USERS,), 0, ITEMS), jax.random.fold_in(keys[2], 1), 0, ITEMS - 1).astype(jnp.int32),
    }


def reference(users, items, pos_ids):
    rows = users.shape[0]
    size = math.gcd(rows, 1024)
    count = rows // size
    bank = items.astype(jnp.float32)
    cols = jnp.arange(items.shape[0], dtype=jnp.int32)

    def step(carry, args):
        ublk, pblk = args
        user_block = ublk.astype(jnp.float32)
        logit = jnp.dot(user_block, bank.T, precision=lax.Precision.HIGHEST)
        mask = pblk[:, None] == cols[None, :]
        peak = jnp.max(logit, axis=1)
        total = jnp.sum(jnp.exp(logit - peak[:, None]), axis=1)
        lse = peak + jnp.log(total)
        positive = jnp.sum(jnp.where(mask, logit, jnp.float32(0.0)), axis=1)
        weights = (jnp.exp(logit - lse[:, None]) - mask.astype(jnp.float32)).astype(jnp.bfloat16)
        weight_full = weights.astype(jnp.float32)
        ugrad = jnp.dot(weight_full, bank, precision=lax.Precision.HIGHEST)
        carry = carry + jnp.dot(weight_full.T, user_block, precision=lax.Precision.HIGHEST)
        return carry, (lse - positive, ugrad)

    start = jnp.zeros(items.shape, jnp.float32)
    item_grad, outputs = lax.scan(step, start, (users.reshape(count, size, users.shape[1]), pos_ids.reshape(count, size)))
    loss = outputs[0].reshape(rows)
    user_grad = outputs[1].reshape(rows, users.shape[1])
    return (loss, user_grad, item_grad)
```

```python
import functools
import math

import jax
import jax.numpy as jnp
from jax import lax
from jax.experimental import pallas as pl
from jax.experimental.pallas import tpu as pltpu
from jax.sharding import PartitionSpec as P

F32 = jnp.float32
BF16 = jnp.bfloat16
MESH = pl.DeviceIdType.MESH
NT = (((1,), (1,)), ((), ()))
TN = (((0,), (0,)), ((), ()))
QUAD = 4
PARTS = 2


def kernel(
    peers, slots, users_ref, items_ref, pos_ref,
    loss_ref, ug_ref, ig_ref, x_recv,
    uall, pall, iall, ucat, e_ref, w_ref, top_ref, part_ref, lse_ref, stat, stat_all,
    term, ug_send, near_recv, far_recv, d_send, d_recv, x_send,
    u_ss, u_rs, p_ss, p_rs, i_ss, i_rs, s_ss, s_rs, g_ss, g_rs, d_ss, d_rs, x_ss, x_rs, in_sem,
):
    own = users_ref.shape[0]
    per = items_ref.shape[0]
    chunks = peers // slots
    batch = lax.axis_index("batch")
    index = lax.axis_index("items")
    core = lax.rem(index, 2)
    me = index // 2
    twin = index + 1 - 2 * core
    other = 1 - batch
    total_index = 2 * peers

    def at(peer):
        return {"batch": batch, "items": 2 * peer + core}

    def peer_at(step):
        return lax.rem(me + step, peers)

    to_twin = {"batch": batch, "items": twin}
    to_other = {"batch": other, "items": index}

    def remote(src, dst, ss, rs, device):
        return pltpu.make_async_remote_copy(
            src_ref=src, dst_ref=dst, send_sem=ss, recv_sem=rs, device_id=device, device_id_type=MESH
        )

    barrier = pltpu.get_barrier_semaphore()

    def steps(count, first, body):
        if count <= 8:
            for step in range(count - 1, first - 1, -1):
                body(step)
        else:
            pl.loop(first, count)(body)

    def each(body):
        steps(peers, 1, body)

    def hello(step):
        pl.semaphore_signal(barrier, inc=1, device_id=at(peer_at(step)), device_id_type=MESH)

    mine_in = (
        pltpu.make_async_copy(items_ref, iall.at[0], in_sem.at[0]),
        pltpu.make_async_copy(users_ref, uall.at[me], in_sem.at[1]),
        pltpu.make_async_copy(pos_ref, pall.at[me], in_sem.at[2]),
    )
    each(hello)
    pl.semaphore_signal(barrier, inc=1, device_id=to_twin, device_id_type=MESH)
    pl.semaphore_signal(barrier, inc=1, device_id=to_other, device_id_type=MESH)
    for copy in mine_in:
        copy.start()
    for copy in mine_in:
        copy.wait()
    pl.semaphore_wait(barrier, peers + 1)

    def users_copy(step, source):
        return remote(uall.at[me], uall.at[source], u_ss.at[step], u_rs.at[source], at(peer_at(step)))

    def pos_copy(step, source):
        return remote(pall.at[me], pall.at[source], p_ss.at[step], p_rs.at[source], at(peer_at(step)))

    def stat_copy(step, source):
        return remote(stat, stat_all.at[source], s_ss.at[step], s_rs.at[source], at(peer_at(step)))

    half = peers // 2
    side = me // half
    place = lax.rem(me, half)

    def near_at(step):
        return side * half + lax.rem(place + step, half)

    def far_at(step):
        return (1 - side) * half + lax.rem(place + step, half)

    def near_copy(step, source):
        peer = near_at(step)
        return remote(term.at[peer], near_recv.at[source], g_ss.at[peer], g_rs.at[source], at(peer))

    def far_copy(step, source):
        peer = far_at(step)
        return remote(ug_send.at[peer], far_recv.at[source], g_ss.at[peer], g_rs.at[source], at(peer))

    def items_copy(src, slot, device):
        return remote(src, iall.at[slot], i_ss.at[slot], i_rs.at[slot], device)

    from_other = items_copy(iall.at[0], 2, to_other)
    from_twin = items_copy(iall.at[0], 1, to_twin)
    from_diag = items_copy(iall.at[2], 3, to_twin)
    from_other.start()
    each(lambda step: pos_copy(step, me).start())
    each(lambda step: users_copy(step, me).start())
    from_twin.start()
    from_other.wait_recv()
    from_diag.start()
    each(lambda step: users_copy(step, peer_at(step)).wait_recv())
    each(lambda step: pos_copy(step, peer_at(step)).wait_recv())

    def over_chunks(body):
        if chunks == 1:
            body(0)
        else:
            pl.loop(0, chunks)(body)

    homes = (
        batch * total_index + index,
        batch * total_index + twin,
        other * total_index + index,
        other * total_index + twin,
    )
    row = lax.broadcasted_iota(jnp.int32, (per, slots * own), 0)

    def ids_of(chunk):
        return jnp.concatenate([pall[chunk * slots + k] for k in range(slots)], axis=1)

    def prepare(chunk):
        ucat[chunk] = jnp.concatenate(
            [uall[chunk * slots + k].astype(F32) for k in range(slots)], axis=0
        ).astype(BF16)

    def forward(q, chunk):
        logit = lax.dot_general(iall[q], ucat[chunk], NT, preferred_element_type=F32)
        top = jnp.max(logit, axis=0, keepdims=True)
        hit = row == ids_of(chunk) - homes[q] * per
        e = jnp.exp(logit - top)
        e_ref[chunk, q] = e
        top_ref[chunk, q] = top
        part_ref[chunk, q, 0:1] = jnp.sum(e, axis=0, keepdims=True)
        part_ref[chunk, q, 1:2] = jnp.sum(jnp.where(hit, logit, 0.0), axis=0, keepdims=True)

    def summarize(chunk):
        tops = top_ref[chunk]
        top = jnp.max(tops, axis=0)
        total = jnp.sum(part_ref[chunk, :, 0:1] * jnp.exp(tops - top[None]), axis=0)
        stat[chunk, 0:1] = top + jnp.log(total)
        stat[chunk, 1:2] = jnp.sum(part_ref[chunk, :, 1:2], axis=0)

    over_chunks(prepare)
    over_chunks(functools.partial(forward, 0))
    from_twin.wait_recv()
    over_chunks(functools.partial(forward, 1))
    over_chunks(functools.partial(forward, 2))
    from_diag.wait_recv()
    over_chunks(functools.partial(forward, 3))
    over_chunks(summarize)
    each(lambda step: stat_copy(step, me).start())
    stat_all[me] = stat[...]
    each(lambda step: stat_copy(step, peer_at(step)).wait_recv())

    def rescale(chunk):
        parts = stat_all[:, chunk]
        lses = parts[:, 0:1]
        peak = jnp.max(lses, axis=0)
        lse = peak + jnp.log(jnp.sum(jnp.exp(lses - peak[None]), axis=0))
        lse_ref[chunk] = lse - jnp.sum(parts[:, 1:2], axis=0)
        top_ref[chunk] = jnp.exp(top_ref[chunk] - lse[None])

    def user_terms(chunk):
        grad = jnp.zeros((slots * own, ucat.shape[2]), F32)
        for q in range(QUAD):
            hit = row == ids_of(chunk) - homes[q] * per
            w = e_ref[chunk, q] * top_ref[chunk, q] - jnp.where(hit, 1.0, 0.0)
            w = w.astype(BF16)
            w_ref[chunk, q] = w
            grad = grad + lax.dot_general(w, iall[q], TN, preferred_element_type=F32)
        for k in range(slots):
            part = grad[k * own : (k + 1) * own]
            term[chunk * slots + k] = part
            ug_send[chunk * slots + k] = part.astype(BF16)

    rows = per // PARTS

    def item_term(q, p):
        def one(chunk):
            return jnp.dot(
                w_ref[chunk, q, p * rows : (p + 1) * rows], ucat[chunk], preferred_element_type=F32
            )

        if chunks == 1:
            return one(0)
        return lax.fori_loop(1, chunks, lambda chunk, acc: acc + one(chunk), one(0))

    def twin_copy(k, p):
        return remote(d_send.at[k, p], d_recv.at[k, p], d_ss.at[k, p], d_rs.at[k, p], to_twin)

    def across_copy(p):
        return remote(x_send.at[p], x_recv.at[p], x_ss.at[p], x_rs.at[p], to_other)

    over_chunks(rescale)
    over_chunks(user_terms)
    steps(half, 0, lambda step: far_copy(step, me).start())
    for p in range(PARTS):
        d_send[0, p] = item_term(3, p)
        twin_copy(0, p).start()
    steps(half, 1, lambda step: near_copy(step, me).start())
    for p in range(PARTS):
        far = item_term(2, p)
        twin_copy(0, p).wait_recv()
        x_send[p] = (far + d_recv[0, p]).astype(BF16)
        across_copy(p).start()
    for p in range(PARTS):
        d_send[1, p] = item_term(1, p)
        twin_copy(1, p).start()
    for p in range(PARTS):
        ig_ref[p * rows : (p + 1) * rows] = item_term(0, p)

    losses = lse_ref[me // slots]
    loss = jnp.zeros((1, own), F32)
    for k in range(slots):
        loss = jnp.where(lax.rem(me, slots) == k, losses[:, k * own : (k + 1) * own], loss)
    loss_ref[...] = loss

    for p in range(PARTS):
        twin_copy(1, p).wait_recv()
        ig_ref[p * rows : (p + 1) * rows] += d_recv[1, p]
    ug_ref[...] = term[me]

    def gather_near(step):
        near_copy(step, near_at(step)).wait_recv()
        ug_ref[...] += near_recv[near_at(step)]

    def gather_far(step):
        far_copy(step, far_at(step)).wait_recv()
        ug_ref[...] += far_recv[far_at(step)].astype(F32)

    steps(half, 1, gather_near)
    steps(half, 0, gather_far)
    for p in range(PARTS):
        across_copy(p).wait_recv()
    from_other.wait_send()
    from_twin.wait_send()
    from_diag.wait_send()
    for p in range(PARTS):
        twin_copy(0, p).wait_send()
        twin_copy(1, p).wait_send()
        across_copy(p).wait_send()
    for copy in (users_copy, pos_copy, stat_copy):
        each(lambda step: copy(step, me).wait_send())
    steps(half, 0, lambda step: far_copy(step, me).wait_send())
    steps(half, 1, lambda step: near_copy(step, me).wait_send())


def settle(loss_in, ug_in, ig_in, x_in, loss_ref, ug_ref, ig_ref):
    loss_ref[...] = loss_in[...]
    ug_ref[...] = ug_in[...]
    rows = x_in.shape[1]
    for p in range(PARTS):
        block = slice(p * rows, (p + 1) * rows)
        ig_ref[block] = ig_in[block] + x_in[p].astype(F32)


def local(users, items, pos_ids):
    own, width = users.shape
    per = items.shape[0]
    peers = lax.axis_size("items") // 2
    slots = math.gcd(peers, 8)
    chunks = peers // slots
    lanes = slots * own
    dma = pltpu.SemaphoreType.DMA
    vmem = pl.BlockSpec(memory_space=pltpu.VMEM)
    hbm = pl.BlockSpec(memory_space=pltpu.HBM)
    loss, user_grad, item_grad, far_terms = pl.pallas_call(
        functools.partial(kernel, peers, slots),
        out_shape=(
            pltpu.VMEM((1, own), F32),
            pltpu.VMEM((own, width), F32),
            pltpu.VMEM((per, width), F32),
            pltpu.VMEM((PARTS, per // PARTS, width), BF16),
        ),
        in_specs=[hbm] * 3,
        out_specs=(vmem, vmem, vmem, vmem),
        scratch_shapes=[
            pltpu.VMEM((peers, own, width), BF16),
            pltpu.VMEM((peers, 1, own), jnp.int32),
            pltpu.VMEM((QUAD, per, width), BF16),
            pltpu.VMEM((chunks, lanes, width), BF16),
            pltpu.VMEM((chunks, QUAD, per, lanes), F32),
            pltpu.VMEM((chunks, QUAD, per, lanes), BF16),
            pltpu.VMEM((chunks, QUAD, 1, lanes), F32),
            pltpu.VMEM((chunks, QUAD, 2, lanes), F32),
            pltpu.VMEM((chunks, 1, lanes), F32),
            pltpu.VMEM((chunks, 2, lanes), F32),
            pltpu.VMEM((peers, chunks, 2, lanes), F32),
            pltpu.VMEM((peers, own, width), F32),
            pltpu.VMEM((peers, own, width), BF16),
            pltpu.VMEM((peers, own, width), F32),
            pltpu.VMEM((peers, own, width), BF16),
            pltpu.VMEM((2, PARTS, per // PARTS, width), F32),
            pltpu.VMEM((2, PARTS, per // PARTS, width), F32),
            pltpu.VMEM((PARTS, per // PARTS, width), BF16),
            dma((peers,)), dma((peers,)),
            dma((peers,)), dma((peers,)),
            dma((QUAD,)), dma((QUAD,)),
            dma((peers,)), dma((peers,)),
            dma((peers,)), dma((peers,)),
            dma((2, PARTS)), dma((2, PARTS)),
            dma((PARTS,)), dma((PARTS,)),
            dma((3,)),
        ],
        compiler_params=pltpu.CompilerParams(
            collective_id=0, has_side_effects=True, vmem_limit_bytes=32 * 1024 * 1024
        ),
    )(*(pltpu.with_memory_space_constraint(v, pltpu.HBM) for v in (users, items, pos_ids.reshape(1, own))))
    loss, user_grad, item_grad = pl.pallas_call(
        settle,
        out_shape=(
            jax.ShapeDtypeStruct((1, own), F32),
            jax.ShapeDtypeStruct((own, width), F32),
            jax.ShapeDtypeStruct((per, width), F32),
        ),
        in_specs=[vmem] * 4,
        out_specs=(vmem,) * 3,
        compiler_params=pltpu.CompilerParams(vmem_limit_bytes=4 * 1024 * 1024),
    )(loss, user_grad, item_grad, far_terms)
    return loss.reshape(own), user_grad, item_grad


def solution(mesh):
    placed = (P(("batch", "items"), None), P(("batch", "items"), None), P(("batch", "items")))
    return jax.shard_map(
        local,
        mesh=mesh,
        in_specs=placed,
        out_specs=(P(("batch", "items")), P(("batch", "items"), None), P(("batch", "items"), None)),
        check_vma=False,
    )
```

```python
import functools
import math

import jax
import jax.numpy as jnp
from jax import lax
from jax.experimental import pallas as pl
from jax.experimental.pallas import tpu as pltpu
from jax.sharding import PartitionSpec as P

F32 = jnp.float32
BF16 = jnp.bfloat16
MESH = pl.DeviceIdType.MESH
NT = (((1,), (1,)), ((), ()))
TN = (((0,), (0,)), ((), ()))
QUAD = 4
PARTS = 2


def kernel(
    peers, slots, users_ref, items_ref, pos_ref,
    loss_ref, ug_ref, ig_ref,
    uall, pall, iall, ucat, e_ref, w_ref, top_ref, part_ref, loss_all, stat, stat_all,
    term, ug_send, near_recv, far_recv, mates, mate_ids, mate_cat, mate_logit, lse_ref, mate_lse,
    u_ss, u_rs, p_ss, p_rs, i_ss, i_rs, s_ss, s_rs, g_ss, g_rs, m_ss, m_rs, n_ss, n_rs, l_ss, l_rs,
    in_sem, ready, x_ready,
):
    own = users_ref.shape[0]
    per = items_ref.shape[0]
    chunks = peers // slots
    batch = lax.axis_index("batch")
    index = lax.axis_index("items")
    core = lax.rem(index, 2)
    me = index // 2
    twin = index + 1 - 2 * core
    other = 1 - batch
    total_index = 2 * peers

    def at(peer):
        return {"batch": batch, "items": 2 * peer + core}

    def peer_at(step):
        return lax.rem(me + step, peers)

    to_twin = {"batch": batch, "items": twin}
    to_other = {"batch": other, "items": index}
    to_diag = {"batch": other, "items": twin}

    def remote(src, dst, ss, rs, device):
        return pltpu.make_async_remote_copy(
            src_ref=src, dst_ref=dst, send_sem=ss, recv_sem=rs, device_id=device, device_id_type=MESH
        )

    barrier = pltpu.get_barrier_semaphore()

    def steps(count, first, body):
        if count <= 8:
            for step in range(count - 1, first - 1, -1):
                body(step)
        else:
            pl.loop(first, count)(body)

    def each(body):
        steps(peers, 1, body)

    def rising(body):
        if peers <= 8:
            for step in range(1, peers):
                body(step)
        else:
            pl.loop(1, peers)(body)

    def greet(step):
        peer = peer_at(step)

        @pl.when(peer > me)
        def _():
            pl.semaphore_signal(barrier, inc=1, device_id=at(peer), device_id_type=MESH)

    def answer(step):
        peer = peer_at(step)

        @pl.when(peer < me)
        def _():
            pl.semaphore_signal(ready.at[me], inc=1, device_id=at(peer), device_id_type=MESH)

    mine_in = (
        pltpu.make_async_copy(items_ref, iall.at[0], in_sem.at[0]),
        pltpu.make_async_copy(users_ref, uall.at[me], in_sem.at[1]),
        pltpu.make_async_copy(pos_ref, pall.at[me], in_sem.at[2]),
    )
    each(greet)
    pl.semaphore_signal(barrier, inc=1, device_id=to_twin, device_id_type=MESH)

    @pl.when(batch == 0)
    def _():
        pl.semaphore_signal(barrier, inc=1, device_id=to_other, device_id_type=MESH)

    for copy in mine_in:
        copy.start()
    pl.semaphore_wait(barrier, me + batch + 1)
    each(answer)

    @pl.when(batch == 1)
    def _():
        pl.semaphore_signal(x_ready.at[0], inc=1, device_id=to_other, device_id_type=MESH)

    for copy in mine_in:
        copy.wait()

    def users_copy(step, source):
        return remote(uall.at[me], uall.at[source], u_ss.at[step], u_rs.at[source], at(peer_at(step)))

    def pos_copy(step, source):
        return remote(pall.at[me], pall.at[source], p_ss.at[step], p_rs.at[source], at(peer_at(step)))

    def stat_copy(step, source):
        return remote(stat, stat_all.at[source], s_ss.at[step], s_rs.at[source], at(peer_at(step)))

    half = peers // 2
    side = me // half
    place = lax.rem(me, half)

    def near_at(step):
        return side * half + lax.rem(place + step, half)

    def far_at(step):
        return (1 - side) * half + lax.rem(place + step, half)

    def near_copy(step, source):
        peer = near_at(step)
        return remote(term.at[peer], near_recv.at[source], g_ss.at[peer], g_rs.at[source], at(peer))

    def far_copy(step, source):
        peer = far_at(step)
        return remote(ug_send.at[peer], far_recv.at[source], g_ss.at[peer], g_rs.at[source], at(peer))

    half_rows = per // PARTS

    def items_copy(source, slot, p, device):
        block = pl.ds(p * half_rows, half_rows)
        return remote(
            iall.at[source, block], iall.at[slot, block], i_ss.at[slot, p], i_rs.at[slot, p], device
        )

    from_other = [items_copy(0, 2, p, to_other) for p in range(PARTS)]
    from_twin = [items_copy(0, 1, p, to_twin) for p in range(PARTS)]
    from_diag = [items_copy(2, 3, p, to_twin) for p in range(PARTS)]

    def send_down(step):
        @pl.when(peer_at(step) < me)
        def _():
            pos_copy(step, me).start()
            users_copy(step, me).start()

    def send_up(step):
        peer = peer_at(step)

        @pl.when(peer > me)
        def _():
            pl.semaphore_wait(ready.at[peer], 1)
            pos_copy(step, me).start()
            users_copy(step, me).start()

    @pl.when(batch == 1)
    def _():
        for copy in from_other:
            copy.start()

    each(send_down)
    for copy in from_twin:
        copy.start()

    @pl.when(batch == 0)
    def _():
        pl.semaphore_wait(x_ready.at[0], 1)
        for copy in from_other:
            copy.start()

    rising(send_up)
    for p in range(PARTS):
        from_other[p].wait_recv()
        from_diag[p].start()
    def near_in(step):
        source = near_at(step)
        users_copy(step, source).wait_recv()
        pos_copy(step, source).wait_recv()

    def far_in(step):
        source = far_at(step)
        users_copy(step, source).wait_recv()
        pos_copy(step, source).wait_recv()

    def mate_copy(src, ids, k, p, part, device):
        block = pl.ds(part * half, half)
        return (
            remote(ids.at[block], mate_ids.at[k, block], n_ss.at[k, p], n_rs.at[k, p], device),
            remote(src.at[block], mates.at[k, block], m_ss.at[k, p], m_rs.at[k, p], device),
        )

    halves = (side, 1 - side)
    to_mates = [
        [mate_copy(uall, pall, 1, p, halves[p], to_other) for p in range(2)],
        [mate_copy(uall, pall, 0, p, halves[p], to_twin) for p in range(2)],
    ]
    onward = [mate_copy(mates.at[1], mate_ids.at[1], 2, p, halves[p], to_twin) for p in range(2)]

    def lend(p):
        for pair in to_mates:
            for copy in pair[p]:
                copy.start()

    steps(half, 1, near_in)
    lend(0)
    steps(half, 0, far_in)
    lend(1)

    def over_chunks(body):
        if chunks == 1:
            body(0)
        else:
            pl.loop(0, chunks)(body)

    homes = (
        batch * total_index + index,
        batch * total_index + twin,
        other * total_index + index,
        other * total_index + twin,
    )
    row = lax.broadcasted_iota(jnp.int32, (per, slots * own), 0)

    def lane_ids(ids, chunk):
        return jnp.concatenate([ids[chunk * slots + k] for k in range(slots)], axis=1)

    def ids_of(chunk):
        return lane_ids(pall, chunk)

    def joined(blocks, chunk):
        return jnp.concatenate(
            [blocks[chunk * slots + k].astype(F32) for k in range(slots)], axis=0
        ).astype(BF16)

    def prepare(chunk):
        ucat[chunk] = joined(uall, chunk)

    def meet(k, chunk):
        mate_cat[k, chunk] = joined(mates.at[k], chunk)
        mate_logit[k, chunk] = lax.dot_general(
            iall[0], mate_cat[k, chunk], NT, preferred_element_type=F32
        )

    def forward(q, chunk):
        logit = lax.dot_general(iall[q], ucat[chunk], NT, preferred_element_type=F32)
        top = jnp.max(logit, axis=0, keepdims=True)
        hit = row == ids_of(chunk) - homes[q] * per
        e = jnp.exp(logit - top)
        e_ref[chunk, q] = e
        top_ref[chunk, q] = top
        part_ref[chunk, q, 0:1] = jnp.sum(e, axis=0, keepdims=True)
        part_ref[chunk, q, 1:2] = jnp.sum(jnp.where(hit, logit, 0.0), axis=0, keepdims=True)

    def summarize(chunk):
        tops = top_ref[chunk]
        top = jnp.max(tops, axis=0)
        total = jnp.sum(part_ref[chunk, :, 0:1] * jnp.exp(tops - top[None]), axis=0)
        stat[chunk, 0:1] = top + jnp.log(total)
        stat[chunk, 1:2] = jnp.sum(part_ref[chunk, :, 1:2], axis=0)

    over_chunks(prepare)
    over_chunks(functools.partial(forward, 0))
    for copy in from_twin:
        copy.wait_recv()
    over_chunks(functools.partial(forward, 1))
    over_chunks(functools.partial(forward, 2))
    for copy in from_diag:
        copy.wait_recv()
    over_chunks(functools.partial(forward, 3))
    over_chunks(summarize)
    each(lambda step: stat_copy(step, me).start())
    stat_all[me] = stat[...]

    def mate_in(k, p):
        for copy in mate_copy(uall, pall, k, p, halves[p], to_twin):
            copy.wait_recv()

    for p in range(2):
        mate_in(0, p)
    over_chunks(functools.partial(meet, 0))
    for p in range(2):
        mate_in(1, p)
        for copy in onward[p]:
            copy.start()
    over_chunks(functools.partial(meet, 1))
    each(lambda step: stat_copy(step, peer_at(step)).wait_recv())

    def rescale(chunk):
        parts = stat_all[:, chunk]
        lses = parts[:, 0:1]
        peak = jnp.max(lses, axis=0)
        lse = peak + jnp.log(jnp.sum(jnp.exp(lses - peak[None]), axis=0))
        lse_ref[chunk] = lse
        loss_all[chunk] = lse - jnp.sum(parts[:, 1:2], axis=0)
        top_ref[chunk] = jnp.exp(top_ref[chunk] - lse[None])

    def user_terms(chunk):
        grad = jnp.zeros((slots * own, ucat.shape[2]), F32)
        for q in range(QUAD):
            hit = row == ids_of(chunk) - homes[q] * per
            w = e_ref[chunk, q] * top_ref[chunk, q] - jnp.where(hit, 1.0, 0.0)
            w = w.astype(BF16)
            w_ref[chunk, q] = w
            grad = grad + lax.dot_general(w, iall[q], TN, preferred_element_type=F32)
        for k in range(slots):
            part = grad[k * own : (k + 1) * own]
            term[chunk * slots + k] = part
            ug_send[chunk * slots + k] = part.astype(BF16)

    def own_term(chunk):
        return jnp.dot(w_ref[chunk, 0], ucat[chunk], preferred_element_type=F32)

    def mate_term(k, chunk):
        hit = row == lane_ids(mate_ids.at[k], chunk) - homes[0] * per
        w = jnp.exp(mate_logit[k, chunk] - mate_lse[k, chunk]) - jnp.where(hit, 1.0, 0.0)
        return jnp.dot(w.astype(BF16), mate_cat[k, chunk], preferred_element_type=F32)

    def total_of(one):
        if chunks == 1:
            return one(0)
        return lax.fori_loop(1, chunks, lambda chunk, acc: acc + one(chunk), one(0))

    lse_copies = [
        remote(lse_ref, mate_lse.at[k], l_ss.at[k], l_rs.at[k], device)
        for k, device in enumerate((to_twin, to_other, to_diag))
    ]

    over_chunks(rescale)
    for copy in (lse_copies[1], lse_copies[2], lse_copies[0]):
        copy.start()
    over_chunks(user_terms)
    steps(half, 0, lambda step: far_copy(step, me).start())
    steps(half, 1, lambda step: near_copy(step, me).start())
    ig_ref[...] = total_of(own_term)
    for p in range(2):
        mate_in(2, p)
    over_chunks(functools.partial(meet, 2))
    for k in range(3):
        lse_copies[k].wait_recv()
        ig_ref[...] += total_of(functools.partial(mate_term, k))

    losses = loss_all[me // slots]
    loss = jnp.zeros((1, own), F32)
    for k in range(slots):
        loss = jnp.where(lax.rem(me, slots) == k, losses[:, k * own : (k + 1) * own], loss)
    loss_ref[...] = loss

    ug_ref[...] = term[me]

    def gather_near(step):
        near_copy(step, near_at(step)).wait_recv()
        ug_ref[...] += near_recv[near_at(step)]

    def gather_far(step):
        far_copy(step, far_at(step)).wait_recv()
        ug_ref[...] += far_recv[far_at(step)].astype(F32)

    steps(half, 1, gather_near)
    steps(half, 0, gather_far)
    for copy in from_other + from_twin + from_diag:
        copy.wait_send()
    for p in range(2):
        for copy in (*to_mates[0][p], *to_mates[1][p], *onward[p]):
            copy.wait_send()
    for copy in lse_copies:
        copy.wait_send()
    for copy in (users_copy, pos_copy, stat_copy):
        each(lambda step: copy(step, me).wait_send())
    steps(half, 0, lambda step: far_copy(step, me).wait_send())
    steps(half, 1, lambda step: near_copy(step, me).wait_send())


def settle(loss_in, ug_in, ig_in, loss_out, ug_out, ig_out, sems):
    copies = [
        pltpu.make_async_copy(src, dst, sems.at[k])
        for k, (src, dst) in enumerate(((ig_in, ig_out), (ug_in, ug_out), (loss_in, loss_out)))
    ]
    for copy in copies:
        copy.start()
    for copy in copies:
        copy.wait()


def local(users, items, pos_ids):
    own, width = users.shape
    per = items.shape[0]
    peers = lax.axis_size("items") // 2
    slots = math.gcd(peers, 8)
    chunks = peers // slots
    lanes = slots * own
    dma = pltpu.SemaphoreType.DMA
    vmem = pl.BlockSpec(memory_space=pltpu.VMEM)
    hbm = pl.BlockSpec(memory_space=pltpu.HBM)
    loss, user_grad, item_grad = pl.pallas_call(
        functools.partial(kernel, peers, slots),
        out_shape=(
            pltpu.VMEM((1, own), F32),
            pltpu.VMEM((own, width), F32),
            pltpu.VMEM((per, width), F32),
        ),
        in_specs=[hbm] * 3,
        out_specs=(vmem, vmem, vmem),
        scratch_shapes=[
            pltpu.VMEM((peers, own, width), BF16),
            pltpu.VMEM((peers, 1, own), jnp.int32),
            pltpu.VMEM((QUAD, per, width), BF16),
            pltpu.VMEM((chunks, lanes, width), BF16),
            pltpu.VMEM((chunks, QUAD, per, lanes), F32),
            pltpu.VMEM((chunks, QUAD, per, lanes), BF16),
            pltpu.VMEM((chunks, QUAD, 1, lanes), F32),
            pltpu.VMEM((chunks, QUAD, 2, lanes), F32),
            pltpu.VMEM((chunks, 1, lanes), F32),
            pltpu.VMEM((chunks, 2, lanes), F32),
            pltpu.VMEM((peers, chunks, 2, lanes), F32),
            pltpu.VMEM((peers, own, width), F32),
            pltpu.VMEM((peers, own, width), BF16),
            pltpu.VMEM((peers, own, width), F32),
            pltpu.VMEM((peers, own, width), BF16),
            pltpu.VMEM((3, peers, own, width), BF16),
            pltpu.VMEM((3, peers, 1, own), jnp.int32),
            pltpu.VMEM((3, chunks, lanes, width), BF16),
            pltpu.VMEM((3, chunks, per, lanes), F32),
            pltpu.VMEM((chunks, 1, lanes), F32),
            pltpu.VMEM((3, chunks, 1, lanes), F32),
            dma((peers,)), dma((peers,)),
            dma((peers,)), dma((peers,)),
            dma((QUAD, PARTS)), dma((QUAD, PARTS)),
            dma((peers,)), dma((peers,)),
            dma((peers,)), dma((peers,)),
            dma((3, 2)), dma((3, 2)),
            dma((3, 2)), dma((3, 2)),
            dma((3,)), dma((3,)),
            dma((3,)),
            pltpu.SemaphoreType.REGULAR((peers,)),
            pltpu.SemaphoreType.REGULAR((1,)),
        ],
        compiler_params=pltpu.CompilerParams(
            collective_id=0, has_side_effects=True, vmem_limit_bytes=48 * 1024 * 1024
        ),
    )(*(pltpu.with_memory_space_constraint(v, pltpu.HBM) for v in (users, items, pos_ids.reshape(1, own))))
    loss, user_grad, item_grad = pl.pallas_call(
        settle,
        out_shape=(
            jax.ShapeDtypeStruct((1, own), F32),
            jax.ShapeDtypeStruct((own, width), F32),
            jax.ShapeDtypeStruct((per, width), F32),
        ),
        in_specs=[vmem] * 3,
        out_specs=(hbm,) * 3,
        scratch_shapes=[dma((3,))],
        compiler_params=pltpu.CompilerParams(vmem_limit_bytes=4 * 1024 * 1024),
    )(loss, user_grad, item_grad)
    return loss.reshape(own), user_grad, item_grad


def solution(mesh):
    placed = (P(("batch", "items"), None), P(("batch", "items"), None), P(("batch", "items")))
    return jax.shard_map(
        local,
        mesh=mesh,
        in_specs=placed,
        out_specs=(P(("batch", "items")), P(("batch", "items"), None), P(("batch", "items"), None)),
        check_vma=False,
    )
```

```python
import functools
import math

import jax
import jax.numpy as jnp
from jax import lax
from jax.experimental import pallas as pl
from jax.experimental.pallas import tpu as pltpu
from jax.sharding import PartitionSpec as P

F32 = jnp.float32
BF16 = jnp.bfloat16
MESH = pl.DeviceIdType.MESH
NT = (((1,), (1,)), ((), ()))
TN = (((0,), (0,)), ((), ()))
QUAD = 4
PARTS = 2


def kernel(
    peers, slots, users_ref, items_ref, pos_ref,
    loss_ref, ug_ref, ig_ref,
    uall, pall, iall, ucat, e_ref, logit_ref, blend, picked, top_ref, part_ref, loss_all, stat, stat_all,
    term, ug_send, near_recv, far_recv, mates, mate_ids, mate_cat, mate_logit, lse_ref, mate_lse,
    u_ss, u_rs, p_ss, p_rs, i_ss, i_rs, s_ss, s_rs, g_ss, g_rs, m_ss, m_rs, n_ss, n_rs, l_ss, l_rs,
    in_sem, ready, x_ready,
):
    own = users_ref.shape[0]
    per = items_ref.shape[0]
    chunks = peers // slots
    batch = lax.axis_index("batch")
    index = lax.axis_index("items")
    core = lax.rem(index, 2)
    me = index // 2
    twin = index + 1 - 2 * core
    other = 1 - batch
    total_index = 2 * peers

    def at(peer):
        return {"batch": batch, "items": 2 * peer + core}

    def peer_at(step):
        return lax.rem(me + step, peers)

    to_twin = {"batch": batch, "items": twin}
    to_other = {"batch": other, "items": index}
    to_diag = {"batch": other, "items": twin}

    def remote(src, dst, ss, rs, device):
        return pltpu.make_async_remote_copy(
            src_ref=src, dst_ref=dst, send_sem=ss, recv_sem=rs, device_id=device, device_id_type=MESH
        )

    barrier = pltpu.get_barrier_semaphore()

    def steps(count, first, body):
        if count <= 8:
            for step in range(count - 1, first - 1, -1):
                body(step)
        else:
            pl.loop(first, count)(body)

    def each(body):
        steps(peers, 1, body)

    def rising(body):
        if peers <= 8:
            for step in range(1, peers):
                body(step)
        else:
            pl.loop(1, peers)(body)

    def greet(step):
        peer = peer_at(step)

        @pl.when(peer > me)
        def _():
            pl.semaphore_signal(barrier, inc=1, device_id=at(peer), device_id_type=MESH)

    def answer(step):
        peer = peer_at(step)

        @pl.when(peer < me)
        def _():
            pl.semaphore_signal(ready.at[me], inc=1, device_id=at(peer), device_id_type=MESH)

    mine_in = (
        pltpu.make_async_copy(items_ref, iall.at[0], in_sem.at[0]),
        pltpu.make_async_copy(users_ref, uall.at[me], in_sem.at[1]),
        pltpu.make_async_copy(pos_ref, pall.at[me], in_sem.at[2]),
    )
    each(greet)
    pl.semaphore_signal(barrier, inc=1, device_id=to_twin, device_id_type=MESH)

    @pl.when(batch == 0)
    def _():
        pl.semaphore_signal(barrier, inc=1, device_id=to_other, device_id_type=MESH)

    for copy in mine_in:
        copy.start()
    pl.semaphore_wait(barrier, me + batch + 1)
    each(answer)

    @pl.when(batch == 1)
    def _():
        pl.semaphore_signal(x_ready.at[0], inc=1, device_id=to_other, device_id_type=MESH)

    for copy in mine_in:
        copy.wait()

    def users_copy(step, source):
        return remote(uall.at[me], uall.at[source], u_ss.at[step], u_rs.at[source], at(peer_at(step)))

    def pos_copy(step, source):
        return remote(pall.at[me], pall.at[source], p_ss.at[step], p_rs.at[source], at(peer_at(step)))

    def stat_copy(step, source):
        return remote(stat, stat_all.at[source], s_ss.at[step], s_rs.at[source], at(peer_at(step)))

    half = peers // 2
    side = me // half
    place = lax.rem(me, half)

    def near_at(step):
        return side * half + lax.rem(place + step, half)

    def far_at(step):
        return (1 - side) * half + lax.rem(place + step, half)

    def near_copy(step, source):
        return to_near(near_at(step), source)

    def far_copy(step, source):
        return to_far(far_at(step), source)

    def to_near(peer, source):
        return remote(term.at[peer], near_recv.at[source], g_ss.at[peer], g_rs.at[source], at(peer))

    def to_far(peer, source):
        return remote(ug_send.at[peer], far_recv.at[source], g_ss.at[peer], g_rs.at[source], at(peer))

    half_rows = per // PARTS

    def items_copy(source, slot, p, device):
        block = pl.ds(p * half_rows, half_rows)
        return remote(
            iall.at[source, block], iall.at[slot, block], i_ss.at[slot, p], i_rs.at[slot, p], device
        )

    from_other = [items_copy(0, 2, p, to_other) for p in range(PARTS)]
    from_twin = [items_copy(0, 1, p, to_twin) for p in range(PARTS)]
    from_diag = [items_copy(2, 3, p, to_twin) for p in range(PARTS)]

    def send_down(step):
        @pl.when(peer_at(step) < me)
        def _():
            pos_copy(step, me).start()
            users_copy(step, me).start()

    def send_up(step):
        peer = peer_at(step)

        @pl.when(peer > me)
        def _():
            pl.semaphore_wait(ready.at[peer], 1)
            pos_copy(step, me).start()
            users_copy(step, me).start()

    @pl.when(batch == 1)
    def _():
        for copy in from_other:
            copy.start()

    each(send_down)
    for copy in from_twin:
        copy.start()

    @pl.when(batch == 0)
    def _():
        pl.semaphore_wait(x_ready.at[0], 1)
        for copy in from_other:
            copy.start()

    rising(send_up)
    for p in range(PARTS):
        from_other[p].wait_recv()
        from_diag[p].start()
    def near_in(step):
        source = near_at(step)
        users_copy(step, source).wait_recv()
        pos_copy(step, source).wait_recv()

    def far_in(step):
        source = far_at(step)
        users_copy(step, source).wait_recv()
        pos_copy(step, source).wait_recv()

    def mate_copy(src, ids, k, p, part, device):
        block = pl.ds(part * half, half)
        return (
            remote(ids.at[block], mate_ids.at[k, block], n_ss.at[k, p], n_rs.at[k, p], device),
            remote(src.at[block], mates.at[k, block], m_ss.at[k, p], m_rs.at[k, p], device),
        )

    halves = (side, 1 - side)
    to_mates = [
        [mate_copy(uall, pall, 1, p, halves[p], to_other) for p in range(2)],
        [mate_copy(uall, pall, 0, p, halves[p], to_twin) for p in range(2)],
    ]
    onward = [mate_copy(mates.at[1], mate_ids.at[1], 2, p, halves[p], to_twin) for p in range(2)]

    def lend(p):
        for pair in to_mates:
            for copy in pair[p]:
                copy.start()

    steps(half, 1, near_in)
    lend(0)
    steps(half, 0, far_in)
    lend(1)

    def over_chunks(body):
        if chunks == 1:
            body(0)
        else:
            pl.loop(0, chunks)(body)

    homes = (
        batch * total_index + index,
        batch * total_index + twin,
        other * total_index + index,
        other * total_index + twin,
    )
    row = lax.broadcasted_iota(jnp.int32, (per, slots * own), 0)

    def lane_ids(ids, chunk):
        return jnp.concatenate([ids[chunk * slots + k] for k in range(slots)], axis=1)

    def ids_of(chunk):
        return lane_ids(pall, chunk)

    def joined(blocks, chunk):
        return jnp.concatenate(
            [blocks[chunk * slots + k].astype(F32) for k in range(slots)], axis=0
        ).astype(BF16)

    def prepare(chunk):
        ucat[chunk] = joined(uall, chunk)

    def meet(k, chunk):
        mate_cat[k, chunk] = joined(mates.at[k], chunk)
        mate_logit[k, chunk] = lax.dot_general(
            iall[0], mate_cat[k, chunk], NT, preferred_element_type=F32
        )

    def forward(q, chunk):
        logit = lax.dot_general(iall[q], ucat[chunk], NT, preferred_element_type=F32)
        top = jnp.max(logit, axis=0, keepdims=True)
        hit = row == ids_of(chunk) - homes[q] * per
        e = jnp.exp(logit - top)
        e_ref[chunk, q] = e.astype(BF16)
        if q == 0:
            logit_ref[chunk] = logit
        top_ref[chunk, q] = top
        part_ref[chunk, q, 0:1] = jnp.sum(e, axis=0, keepdims=True)
        part_ref[chunk, q, 1:2] = jnp.sum(jnp.where(hit, logit, 0.0), axis=0, keepdims=True)

    def summarize(chunk):
        tops = top_ref[chunk]
        top = jnp.max(tops, axis=0)
        total = jnp.sum(part_ref[chunk, :, 0:1] * jnp.exp(tops - top[None]), axis=0)
        stat[chunk, 0:1] = top + jnp.log(total)
        stat[chunk, 1:2] = jnp.sum(part_ref[chunk, :, 1:2], axis=0)

    over_chunks(prepare)
    over_chunks(functools.partial(forward, 0))
    for copy in from_twin:
        copy.wait_recv()
    over_chunks(functools.partial(forward, 1))
    over_chunks(functools.partial(forward, 2))
    for copy in from_diag:
        copy.wait_recv()
    over_chunks(functools.partial(forward, 3))
    over_chunks(summarize)
    each(lambda step: stat_copy(step, me).start())
    stat_all[me] = stat[...]

    def mate_in(k, p):
        for copy in mate_copy(uall, pall, k, p, halves[p], to_twin):
            copy.wait_recv()

    def columns(rows):
        return jnp.transpose(jnp.concatenate([rows] * (8 // rows.shape[0]), axis=0))

    def gather_terms(chunk):
        share = columns(
            jnp.concatenate([top_ref[chunk, q] - stat[chunk, 0:1] for q in range(QUAD)], axis=0)
        )
        mix = jnp.zeros((slots * own, ucat.shape[2]), F32)
        pick = jnp.zeros((slots * own, ucat.shape[2]), F32)
        for q in range(QUAD):
            hit = jnp.where(row == ids_of(chunk) - homes[q] * per, 1.0, 0.0).astype(BF16)
            part = lax.dot_general(e_ref[chunk, q], iall[q], TN, preferred_element_type=F32)
            mix = mix + part * jnp.exp(share[:, q : q + 1])
            pick = pick + lax.dot_general(hit, iall[q], TN, preferred_element_type=F32)
        blend[chunk] = mix
        picked[chunk] = pick

    over_chunks(gather_terms)
    for p in range(2):
        mate_in(0, p)
    over_chunks(functools.partial(meet, 0))
    for p in range(2):
        mate_in(1, p)
        for copy in onward[p]:
            copy.start()
    over_chunks(functools.partial(meet, 1))
    for copy in from_other + from_twin + from_diag:
        copy.wait_send()
    for copy in (users_copy, pos_copy):
        each(lambda step: copy(step, me).wait_send())
    each(lambda step: stat_copy(step, peer_at(step)).wait_recv())


    def rescale(chunk):
        parts = stat_all[:, chunk]
        lses = parts[:, 0:1]
        peak = jnp.max(lses, axis=0)
        lse = peak + jnp.log(jnp.sum(jnp.exp(lses - peak[None]), axis=0))
        lse_ref[chunk] = lse
        loss_all[chunk] = lse - jnp.sum(parts[:, 1:2], axis=0)

    def user_terms(chunk):
        share = columns(stat[chunk, 0:1] - lse_ref[chunk])[:, 0:1]
        grad = blend[chunk] * jnp.exp(share) - picked[chunk]
        for k in range(slots):
            part = grad[k * own : (k + 1) * own]
            term[chunk * slots + k] = part
            ug_send[chunk * slots + k] = part.astype(BF16)

    def own_term(chunk):
        hit = row == ids_of(chunk) - homes[0] * per
        w = jnp.exp(logit_ref[chunk] - lse_ref[chunk]) - jnp.where(hit, 1.0, 0.0)
        return jnp.dot(w.astype(BF16), ucat[chunk], preferred_element_type=F32)

    def mate_term(k, chunk):
        hit = row == lane_ids(mate_ids.at[k], chunk) - homes[0] * per
        w = jnp.exp(mate_logit[k, chunk] - mate_lse[k, chunk]) - jnp.where(hit, 1.0, 0.0)
        return jnp.dot(w.astype(BF16), mate_cat[k, chunk], preferred_element_type=F32)

    def total_of(one):
        if chunks == 1:
            return one(0)
        return lax.fori_loop(1, chunks, lambda chunk, acc: acc + one(chunk), one(0))

    lse_copies = [
        remote(lse_ref, mate_lse.at[k], l_ss.at[k], l_rs.at[k], device)
        for k, device in enumerate((to_twin, to_other, to_diag))
    ]

    over_chunks(rescale)
    for copy in (lse_copies[1], lse_copies[2], lse_copies[0]):
        copy.start()
    over_chunks(user_terms)
    def low_first(body):
        if peers <= 8:
            for peer in range(peers):
                body(peer)
        else:
            pl.loop(0, peers)(body)

    def give(peer):
        @pl.when(peer // half != side)
        def _():
            to_far(peer, me).start()

        @pl.when(jnp.logical_and(peer // half == side, peer != me))
        def _():
            to_near(peer, me).start()

    low_first(give)
    ig_ref[...] = total_of(own_term)
    for p in range(2):
        mate_in(2, p)
    over_chunks(functools.partial(meet, 2))
    each(lambda step: stat_copy(step, me).wait_send())
    for p in range(2):
        for copy in (*to_mates[0][p], *to_mates[1][p], *onward[p]):
            copy.wait_send()
    for copy in lse_copies:
        copy.wait_send()
    for k in range(3):
        lse_copies[k].wait_recv()
        ig_ref[...] += total_of(functools.partial(mate_term, k))

    losses = loss_all[me // slots]
    loss = jnp.zeros((1, own), F32)
    for k in range(slots):
        loss = jnp.where(lax.rem(me, slots) == k, losses[:, k * own : (k + 1) * own], loss)
    loss_ref[...] = loss

    ug_ref[...] = term[me]

    def gather_near(step):
        near_copy(step, near_at(step)).wait_recv()
        ug_ref[...] += near_recv[near_at(step)]

    def gather_far(step):
        far_copy(step, far_at(step)).wait_recv()
        ug_ref[...] += far_recv[far_at(step)].astype(F32)

    steps(half, 1, gather_near)
    steps(half, 0, gather_far)
    steps(half, 0, lambda step: far_copy(step, me).wait_send())
    steps(half, 1, lambda step: near_copy(step, me).wait_send())


def settle(loss_in, ug_in, ig_in, loss_out, ug_out, ig_out, sems):
    copies = [
        pltpu.make_async_copy(src, dst, sems.at[k])
        for k, (src, dst) in enumerate(((ig_in, ig_out), (ug_in, ug_out), (loss_in, loss_out)))
    ]
    for copy in copies:
        copy.start()
    for copy in copies:
        copy.wait()


def local(users, items, pos_ids):
    own, width = users.shape
    per = items.shape[0]
    peers = lax.axis_size("items") // 2
    slots = math.gcd(peers, 8)
    chunks = peers // slots
    lanes = slots * own
    dma = pltpu.SemaphoreType.DMA
    vmem = pl.BlockSpec(memory_space=pltpu.VMEM)
    hbm = pl.BlockSpec(memory_space=pltpu.HBM)
    loss, user_grad, item_grad = pl.pallas_call(
        functools.partial(kernel, peers, slots),
        out_shape=(
            pltpu.VMEM((1, own), F32),
            pltpu.VMEM((own, width), F32),
            pltpu.VMEM((per, width), F32),
        ),
        in_specs=[hbm] * 3,
        out_specs=(vmem, vmem, vmem),
        scratch_shapes=[
            pltpu.VMEM((peers, own, width), BF16),
            pltpu.VMEM((peers, 1, own), jnp.int32),
            pltpu.VMEM((QUAD, per, width), BF16),
            pltpu.VMEM((chunks, lanes, width), BF16),
            pltpu.VMEM((chunks, QUAD, per, lanes), BF16),
            pltpu.VMEM((chunks, per, lanes), F32),
            pltpu.VMEM((chunks, lanes, width), F32),
            pltpu.VMEM((chunks, lanes, width), F32),
            pltpu.VMEM((chunks, QUAD, 1, lanes), F32),
            pltpu.VMEM((chunks, QUAD, 2, lanes), F32),
            pltpu.VMEM((chunks, 1, lanes), F32),
            pltpu.VMEM((chunks, 2, lanes), F32),
            pltpu.VMEM((peers, chunks, 2, lanes), F32),
            pltpu.VMEM((peers, own, width), F32),
            pltpu.VMEM((peers, own, width), BF16),
            pltpu.VMEM((peers, own, width), F32),
            pltpu.VMEM((peers, own, width), BF16),
            pltpu.VMEM((3, peers, own, width), BF16),
            pltpu.VMEM((3, peers, 1, own), jnp.int32),
            pltpu.VMEM((3, chunks, lanes, width), BF16),
            pltpu.VMEM((3, chunks, per, lanes), F32),
            pltpu.VMEM((chunks, 1, lanes), F32),
            pltpu.VMEM((3, chunks, 1, lanes), F32),
            dma((peers,)), dma((peers,)),
            dma((peers,)), dma((peers,)),
            dma((QUAD, PARTS)), dma((QUAD, PARTS)),
            dma((peers,)), dma((peers,)),
            dma((peers,)), dma((peers,)),
            dma((3, 2)), dma((3, 2)),
            dma((3, 2)), dma((3, 2)),
            dma((3,)), dma((3,)),
            dma((3,)),
            pltpu.SemaphoreType.REGULAR((peers,)),
            pltpu.SemaphoreType.REGULAR((1,)),
        ],
        compiler_params=pltpu.CompilerParams(
            collective_id=0, has_side_effects=True, vmem_limit_bytes=48 * 1024 * 1024
        ),
    )(*(pltpu.with_memory_space_constraint(v, pltpu.HBM) for v in (users, items, pos_ids.reshape(1, own))))
    loss, user_grad, item_grad = pl.pallas_call(
        settle,
        out_shape=(
            jax.ShapeDtypeStruct((1, own), F32),
            jax.ShapeDtypeStruct((own, width), F32),
            jax.ShapeDtypeStruct((per, width), F32),
        ),
        in_specs=[vmem] * 3,
        out_specs=(hbm,) * 3,
        scratch_shapes=[dma((3,))],
        compiler_params=pltpu.CompilerParams(vmem_limit_bytes=4 * 1024 * 1024),
    )(loss, user_grad, item_grad)
    return loss.reshape(own), user_grad, item_grad


def solution(mesh):
    placed = (P(("batch", "items"), None), P(("batch", "items"), None), P(("batch", "items")))
    return jax.shard_map(
        local,
        mesh=mesh,
        in_specs=placed,
        out_specs=(P(("batch", "items")), P(("batch", "items"), None), P(("batch", "items"), None)),
        check_vma=False,
    )
```

```python
import functools
import math

import jax
import jax.numpy as jnp
from jax import lax
from jax.experimental import pallas as pl
from jax.experimental.pallas import tpu as pltpu
from jax.sharding import PartitionSpec as P

F32 = jnp.float32
BF16 = jnp.bfloat16
MESH = pl.DeviceIdType.MESH
NT = (((1,), (1,)), ((), ()))
TN = (((0,), (0,)), ((), ()))
QUAD = 4
PARTS = 2


def kernel(
    peers, slots, users_ref, items_ref, pos_ref,
    loss_ref, ug_ref, ig_ref,
    uall, pall, iall, ucat, e_ref, logit_ref, blend, picked, total_ref, stat, stat_all, pos, pos_all,
    term, ug_send, near_recv, far_recv, mates, mate_ids, mate_cat, mate_logit, lse_ref, mate_lse,
    u_ss, u_rs, p_ss, p_rs, i_ss, i_rs, s_ss, s_rs, h_ss, h_rs, g_ss, g_rs, m_ss, m_rs, n_ss, n_rs, l_ss, l_rs,
    in_sem, ready, x_ready,
):
    own = users_ref.shape[0]
    per = items_ref.shape[0]
    chunks = peers // slots
    batch = lax.axis_index("batch")
    index = lax.axis_index("items")
    core = lax.rem(index, 2)
    me = index // 2
    twin = index + 1 - 2 * core
    other = 1 - batch
    total_index = 2 * peers

    def at(peer):
        return {"batch": batch, "items": 2 * peer + core}

    def peer_at(step):
        return lax.rem(me + step, peers)

    to_twin = {"batch": batch, "items": twin}
    to_other = {"batch": other, "items": index}
    to_diag = {"batch": other, "items": twin}

    def remote(src, dst, ss, rs, device):
        return pltpu.make_async_remote_copy(
            src_ref=src, dst_ref=dst, send_sem=ss, recv_sem=rs, device_id=device, device_id_type=MESH
        )

    barrier = pltpu.get_barrier_semaphore()

    def steps(count, first, body):
        if count <= 8:
            for step in range(count - 1, first - 1, -1):
                body(step)
        else:
            pl.loop(first, count)(body)

    def each(body):
        steps(peers, 1, body)

    def rising(body):
        if peers <= 8:
            for step in range(1, peers):
                body(step)
        else:
            pl.loop(1, peers)(body)

    def greet(step):
        peer = peer_at(step)

        @pl.when(peer > me)
        def _():
            pl.semaphore_signal(barrier, inc=1, device_id=at(peer), device_id_type=MESH)

    def answer(step):
        peer = peer_at(step)

        @pl.when(peer < me)
        def _():
            pl.semaphore_signal(ready.at[me], inc=1, device_id=at(peer), device_id_type=MESH)

    mine_in = (
        pltpu.make_async_copy(items_ref, iall.at[0], in_sem.at[0]),
        pltpu.make_async_copy(users_ref, uall.at[me], in_sem.at[1]),
        pltpu.make_async_copy(pos_ref, pall.at[me], in_sem.at[2]),
    )
    each(greet)
    pl.semaphore_signal(barrier, inc=1, device_id=to_twin, device_id_type=MESH)

    @pl.when(batch == 0)
    def _():
        pl.semaphore_signal(barrier, inc=1, device_id=to_other, device_id_type=MESH)

    for copy in mine_in:
        copy.start()
    pl.semaphore_wait(barrier, me + batch + 1)
    each(answer)

    @pl.when(batch == 1)
    def _():
        pl.semaphore_signal(x_ready.at[0], inc=1, device_id=to_other, device_id_type=MESH)

    for copy in mine_in:
        copy.wait()

    def users_copy(step, source):
        return remote(uall.at[me], uall.at[source], u_ss.at[step], u_rs.at[source], at(peer_at(step)))

    def pos_copy(step, source):
        return remote(pall.at[me], pall.at[source], p_ss.at[step], p_rs.at[source], at(peer_at(step)))

    def stat_copy(step, source):
        return remote(stat, stat_all.at[source], s_ss.at[step], s_rs.at[source], at(peer_at(step)))

    half = peers // 2
    side = me // half
    place = lax.rem(me, half)

    def near_at(step):
        return side * half + lax.rem(place + step, half)

    def far_at(step):
        return (1 - side) * half + lax.rem(place + step, half)

    def near_copy(step, source):
        return to_near(near_at(step), source)

    def far_copy(step, source):
        return to_far(far_at(step), source)

    def to_near(peer, source):
        return remote(term.at[peer], near_recv.at[source], g_ss.at[peer], g_rs.at[source], at(peer))

    def to_far(peer, source):
        return remote(ug_send.at[peer], far_recv.at[source], g_ss.at[peer], g_rs.at[source], at(peer))

    half_rows = per // PARTS

    def items_copy(source, slot, p, device):
        block = pl.ds(p * half_rows, half_rows)
        return remote(
            iall.at[source, block], iall.at[slot, block], i_ss.at[slot, p], i_rs.at[slot, p], device
        )

    from_other = [items_copy(0, 2, p, to_other) for p in range(PARTS)]
    from_twin = [items_copy(0, 1, p, to_twin) for p in range(PARTS)]
    from_diag = [items_copy(2, 3, p, to_twin) for p in range(PARTS)]

    def send_down(step):
        @pl.when(peer_at(step) < me)
        def _():
            pos_copy(step, me).start()
            users_copy(step, me).start()

    def send_up(step):
        peer = peer_at(step)

        @pl.when(peer > me)
        def _():
            pl.semaphore_wait(ready.at[peer], 1)
            pos_copy(step, me).start()
            users_copy(step, me).start()

    @pl.when(batch == 1)
    def _():
        for copy in from_other:
            copy.start()

    each(send_down)
    for copy in from_twin:
        copy.start()

    @pl.when(batch == 0)
    def _():
        pl.semaphore_wait(x_ready.at[0], 1)
        for copy in from_other:
            copy.start()

    rising(send_up)
    for p in range(PARTS):
        from_other[p].wait_recv()
        from_diag[p].start()
    def near_in(step):
        source = near_at(step)
        users_copy(step, source).wait_recv()
        pos_copy(step, source).wait_recv()

    def far_in(step):
        source = far_at(step)
        users_copy(step, source).wait_recv()
        pos_copy(step, source).wait_recv()

    def mate_copy(src, ids, k, p, part, device):
        block = pl.ds(part * half, half)
        return (
            remote(ids.at[block], mate_ids.at[k, block], n_ss.at[k, p], n_rs.at[k, p], device),
            remote(src.at[block], mates.at[k, block], m_ss.at[k, p], m_rs.at[k, p], device),
        )

    halves = (side, 1 - side)
    to_mates = [
        [mate_copy(uall, pall, 1, p, halves[p], to_other) for p in range(2)],
        [mate_copy(uall, pall, 0, p, halves[p], to_twin) for p in range(2)],
    ]
    onward = [mate_copy(mates.at[1], mate_ids.at[1], 2, p, halves[p], to_twin) for p in range(2)]

    def lend(p):
        for pair in to_mates:
            for copy in pair[p]:
                copy.start()

    steps(half, 1, near_in)
    lend(0)

    def over_chunks(body):
        if chunks <= 2:
            for chunk in range(chunks):
                body(chunk)
        else:
            pl.loop(0, chunks)(body)

    def over_half(which, body):
        count = chunks // 2
        if count == 1:
            body(which)
        else:
            pl.loop(0, count)(lambda chunk: body(which * count + chunk))

    homes = (
        batch * total_index + index,
        batch * total_index + twin,
        other * total_index + index,
        other * total_index + twin,
    )
    row = lax.broadcasted_iota(jnp.int32, (per, slots * own), 0)

    def lane_ids(ids, chunk):
        return jnp.concatenate([ids[chunk * slots + k] for k in range(slots)], axis=1)

    def ids_of(chunk):
        return lane_ids(pall, chunk)

    def joined(blocks, chunk):
        return jnp.concatenate(
            [blocks[chunk * slots + k].astype(F32) for k in range(slots)], axis=0
        ).astype(BF16)

    def prepare(chunk):
        ucat[chunk] = joined(uall, chunk)

    def meet(k, chunk):
        mate_cat[k, chunk] = joined(mates.at[k], chunk)
        mate_logit[k, chunk] = lax.dot_general(
            iall[0], mate_cat[k, chunk], NT, preferred_element_type=F32
        )

    def forward(chunk):
        items = iall[...].reshape(QUAD * per, iall.shape[2])
        logit = lax.dot_general(items, ucat[chunk], NT, preferred_element_type=F32)
        top = jnp.max(logit, axis=0, keepdims=True)
        e = jnp.exp(logit - top)
        total = jnp.sum(e, axis=0, keepdims=True)
        stat[chunk] = top + jnp.log(total)
        total_ref[chunk] = total
        e_ref[chunk] = e.astype(BF16)
        logit_ref[chunk] = logit[:per]

    for copy in from_twin + from_diag:
        copy.wait_recv()

    def advance(chunk):
        prepare(chunk)
        forward(chunk)

    over_half(side, advance)
    steps(half, 0, far_in)
    over_half(1 - side, advance)
    each(lambda step: stat_copy(step, me).start())
    stat_all[me] = stat[...]
    lend(1)

    def mate_in(k, p):
        for copy in mate_copy(uall, pall, k, p, halves[p], to_twin):
            copy.wait_recv()

    def columns(rows):
        return jnp.transpose(jnp.concatenate([rows] * (8 // rows.shape[0]), axis=0))

    def gather_terms(chunk):
        share = 1.0 / columns(total_ref[chunk])[:, 0:1]
        mix = jnp.zeros((slots * own, ucat.shape[2]), F32)
        pick = jnp.zeros((slots * own, ucat.shape[2]), F32)
        for q in range(QUAD):
            here = row == ids_of(chunk) - homes[q] * per
            hit = jnp.where(here, 1.0, 0.0).astype(BF16)
            rest = jnp.where(here, 0.0, e_ref[chunk, q * per : (q + 1) * per].astype(F32)).astype(BF16)
            part = lax.dot_general(rest, iall[q], TN, preferred_element_type=F32)
            mix = mix + part
            pick = pick + lax.dot_general(hit, iall[q], TN, preferred_element_type=F32)
        blend[chunk] = mix * share
        picked[chunk] = pick
        pos[chunk] = lax.dot_general(
            jnp.ones((8, pick.shape[1]), F32), ucat[chunk].astype(F32) * pick, NT,
            precision=lax.Precision.HIGHEST, preferred_element_type=F32,
        )[0:1]

    def pos_out(step, source):
        return remote(pos, pos_all.at[source], h_ss.at[step], h_rs.at[source], at(peer_at(step)))

    over_chunks(gather_terms)
    each(lambda step: pos_out(step, me).start())
    pos_all[me] = pos[...]
    for p in range(2):
        mate_in(0, p)
    over_chunks(functools.partial(meet, 0))
    mate_in(1, 0)
    for copy in onward[0]:
        copy.start()
    for copy in from_other + from_twin + from_diag:
        copy.wait_send()
    for copy in (users_copy, pos_copy):
        each(lambda step: copy(step, me).wait_send())
    each(lambda step: stat_copy(step, peer_at(step)).wait_recv())


    def rescale(chunk):
        lses = stat_all[:, chunk]
        peak = jnp.max(lses, axis=0)
        lse_ref[chunk] = peak + jnp.log(jnp.sum(jnp.exp(lses - peak[None]), axis=0))

    def user_terms(chunk):
        lse = lse_ref[chunk]
        at_pos = jnp.exp(jnp.minimum(pos[chunk] - lse, 0.0)) - 1.0
        scale = columns(
            jnp.concatenate([jnp.exp(stat[chunk] - lse), at_pos.astype(BF16).astype(F32)], axis=0)
        )
        grad = blend[chunk] * scale[:, 0:1] + picked[chunk] * scale[:, 1:2]
        for k in range(slots):
            part = grad[k * own : (k + 1) * own]
            term[chunk * slots + k] = part
            ug_send[chunk * slots + k] = part.astype(BF16)

    def own_term(chunk):
        hit = row == ids_of(chunk) - homes[0] * per
        w = jnp.exp(logit_ref[chunk] - lse_ref[chunk]) - jnp.where(hit, 1.0, 0.0)
        return jnp.dot(w.astype(BF16), ucat[chunk], preferred_element_type=F32)

    def mate_term(k, chunk):
        hit = row == lane_ids(mate_ids.at[k], chunk) - homes[0] * per
        w = jnp.exp(mate_logit[k, chunk] - mate_lse[k, chunk]) - jnp.where(hit, 1.0, 0.0)
        return jnp.dot(w.astype(BF16), mate_cat[k, chunk], preferred_element_type=F32)

    def total_of(one):
        if chunks == 2:
            return one(0) + one(1)
        return lax.fori_loop(1, chunks, lambda chunk, acc: acc + one(chunk), one(0))

    lse_copies = [
        remote(lse_ref, mate_lse.at[k], l_ss.at[k], l_rs.at[k], device)
        for k, device in enumerate((to_twin, to_other, to_diag))
    ]

    over_chunks(rescale)
    for copy in (lse_copies[1], lse_copies[2], lse_copies[0]):
        copy.start()
    over_chunks(user_terms)
    def low_first(body):
        if peers <= 8:
            for peer in range(peers):
                body(peer)
        else:
            pl.loop(0, peers)(body)

    def give(peer):
        @pl.when(peer // half != side)
        def _():
            to_far(peer, me).start()

        @pl.when(jnp.logical_and(peer // half == side, peer != me))
        def _():
            to_near(peer, me).start()

    low_first(give)
    ig_ref[...] = total_of(own_term)
    mate_in(1, 1)
    for copy in onward[1]:
        copy.start()
    over_chunks(functools.partial(meet, 1))
    for p in range(2):
        mate_in(2, p)
    over_chunks(functools.partial(meet, 2))
    each(lambda step: stat_copy(step, me).wait_send())
    each(lambda step: pos_out(step, me).wait_send())
    for p in range(2):
        for copy in (*to_mates[0][p], *to_mates[1][p], *onward[p]):
            copy.wait_send()
    for copy in lse_copies:
        copy.wait_send()
    for k in (0, 2, 1):
        lse_copies[k].wait_recv()
        ig_ref[...] += total_of(functools.partial(mate_term, k))

    each(lambda step: pos_out(step, peer_at(step)).wait_recv())
    losses = lse_ref[me // slots] - jnp.sum(pos_all[:, me // slots], axis=0)
    loss = jnp.zeros((1, own), F32)
    for k in range(slots):
        loss = jnp.where(lax.rem(me, slots) == k, losses[:, k * own : (k + 1) * own], loss)
    loss_ref[...] = loss

    ug_ref[...] = term[me]

    def gather_near(step):
        near_copy(step, near_at(step)).wait_recv()
        ug_ref[...] += near_recv[near_at(step)]

    def gather_far(step):
        far_copy(step, far_at(step)).wait_recv()
        ug_ref[...] += far_recv[far_at(step)].astype(F32)

    steps(half, 1, gather_near)
    steps(half, 0, gather_far)
    steps(half, 0, lambda step: far_copy(step, me).wait_send())
    steps(half, 1, lambda step: near_copy(step, me).wait_send())


def settle(loss_in, ug_in, ig_in, loss_out, ug_out, ig_out, sems):
    copies = [
        pltpu.make_async_copy(src, dst, sems.at[k])
        for k, (src, dst) in enumerate(((ig_in, ig_out), (ug_in, ug_out), (loss_in, loss_out)))
    ]
    for copy in copies:
        copy.start()
    for copy in copies:
        copy.wait()


def local(users, items, pos_ids):
    own, width = users.shape
    per = items.shape[0]
    peers = lax.axis_size("items") // 2
    slots = math.gcd(peers // 2, 4)
    chunks = peers // slots
    lanes = slots * own
    dma = pltpu.SemaphoreType.DMA
    vmem = pl.BlockSpec(memory_space=pltpu.VMEM)
    hbm = pl.BlockSpec(memory_space=pltpu.HBM)
    loss, user_grad, item_grad = pl.pallas_call(
        functools.partial(kernel, peers, slots),
        out_shape=(
            pltpu.VMEM((1, own), F32),
            pltpu.VMEM((own, width), F32),
            pltpu.VMEM((per, width), F32),
        ),
        in_specs=[hbm] * 3,
        out_specs=(vmem, vmem, vmem),
        scratch_shapes=[
            pltpu.VMEM((peers, own, width), BF16),
            pltpu.VMEM((peers, 1, own), jnp.int32),
            pltpu.VMEM((QUAD, per, width), BF16),
            pltpu.VMEM((chunks, lanes, width), BF16),
            pltpu.VMEM((chunks, QUAD * per, lanes), BF16),
            pltpu.VMEM((chunks, per, lanes), F32),
            pltpu.VMEM((chunks, lanes, width), F32),
            pltpu.VMEM((chunks, lanes, width), F32),
            pltpu.VMEM((chunks, 1, lanes), F32),
            pltpu.VMEM((chunks, 1, lanes), F32),
            pltpu.VMEM((peers, chunks, 1, lanes), F32),
            pltpu.VMEM((chunks, 1, lanes), F32),
            pltpu.VMEM((peers, chunks, 1, lanes), F32),
            pltpu.VMEM((peers, own, width), F32),
            pltpu.VMEM((peers, own, width), BF16),
            pltpu.VMEM((peers, own, width), F32),
            pltpu.VMEM((peers, own, width), BF16),
            pltpu.VMEM((3, peers, own, width), BF16),
            pltpu.VMEM((3, peers, 1, own), jnp.int32),
            pltpu.VMEM((3, chunks, lanes, width), BF16),
            pltpu.VMEM((3, chunks, per, lanes), F32),
            pltpu.VMEM((chunks, 1, lanes), F32),
            pltpu.VMEM((3, chunks, 1, lanes), F32),
            dma((peers,)), dma((peers,)),
            dma((peers,)), dma((peers,)),
            dma((QUAD, PARTS)), dma((QUAD, PARTS)),
            dma((peers,)), dma((peers,)),
            dma((peers,)), dma((peers,)),
            dma((peers,)), dma((peers,)),
            dma((3, 2)), dma((3, 2)),
            dma((3, 2)), dma((3, 2)),
            dma((3,)), dma((3,)),
            dma((3,)),
            pltpu.SemaphoreType.REGULAR((peers,)),
            pltpu.SemaphoreType.REGULAR((1,)),
        ],
        compiler_params=pltpu.CompilerParams(
            collective_id=0, has_side_effects=True, vmem_limit_bytes=56 * 1024 * 1024
        ),
    )(*(pltpu.with_memory_space_constraint(v, pltpu.HBM) for v in (users, items, pos_ids.reshape(1, own))))
    loss, user_grad, item_grad = pl.pallas_call(
        settle,
        out_shape=(
            jax.ShapeDtypeStruct((1, own), F32),
            jax.ShapeDtypeStruct((own, width), F32),
            jax.ShapeDtypeStruct((per, width), F32),
        ),
        in_specs=[vmem] * 3,
        out_specs=(hbm,) * 3,
        scratch_shapes=[dma((3,))],
        compiler_params=pltpu.CompilerParams(vmem_limit_bytes=4 * 1024 * 1024),
    )(loss, user_grad, item_grad)
    return loss.reshape(own), user_grad, item_grad


def solution(mesh):
    placed = (P(("batch", "items"), None), P(("batch", "items"), None), P(("batch", "items")))
    return jax.shard_map(
        local,
        mesh=mesh,
        in_specs=placed,
        out_specs=(P(("batch", "items")), P(("batch", "items"), None), P(("batch", "items"), None)),
        check_vma=False,
    )
```

```python
import functools
import math

import jax
import jax.numpy as jnp
from jax import lax
from jax.experimental import pallas as pl
from jax.experimental.pallas import tpu as pltpu
from jax.sharding import PartitionSpec as P

F32 = jnp.float32
BF16 = jnp.bfloat16
MESH = pl.DeviceIdType.MESH
NT = (((1,), (1,)), ((), ()))
TN = (((0,), (0,)), ((), ()))
QUAD = 4
PARTS = 2


def kernel(
    peers, slots, users_ref, items_ref, pos_ref,
    loss_ref, ug_ref, ig_ref,
    uall, pall, iall, ucat, e_ref, logit_ref, blend, picked, top_ref, stat, stat_all, pos, pos_all,
    term, ug_send, near_recv, far_recv, mates, mate_ids, mate_cat, mate_logit, lse_ref, mate_lse,
    u_ss, u_rs, p_ss, p_rs, i_ss, i_rs, s_ss, s_rs, h_ss, h_rs, g_ss, g_rs, m_ss, m_rs, n_ss, n_rs, l_ss, l_rs,
    in_sem, ready, x_ready,
):
    own = users_ref.shape[0]
    per = items_ref.shape[0]
    chunks = peers // slots
    batch = lax.axis_index("batch")
    index = lax.axis_index("items")
    core = lax.rem(index, 2)
    me = index // 2
    twin = index + 1 - 2 * core
    other = 1 - batch
    total_index = 2 * peers

    def at(peer):
        return {"batch": batch, "items": 2 * peer + core}

    def peer_at(step):
        return lax.rem(me + step, peers)

    to_twin = {"batch": batch, "items": twin}
    to_other = {"batch": other, "items": index}
    to_diag = {"batch": other, "items": twin}

    def remote(src, dst, ss, rs, device):
        return pltpu.make_async_remote_copy(
            src_ref=src, dst_ref=dst, send_sem=ss, recv_sem=rs, device_id=device, device_id_type=MESH
        )

    barrier = pltpu.get_barrier_semaphore()

    def steps(count, first, body):
        if count <= 8:
            for step in range(count - 1, first - 1, -1):
                body(step)
        else:
            pl.loop(first, count)(body)

    def each(body):
        steps(peers, 1, body)

    def rising(body):
        if peers <= 8:
            for step in range(1, peers):
                body(step)
        else:
            pl.loop(1, peers)(body)

    def greet(step):
        peer = peer_at(step)

        @pl.when(peer > me)
        def _():
            pl.semaphore_signal(barrier, inc=1, device_id=at(peer), device_id_type=MESH)

    def answer(step):
        peer = peer_at(step)

        @pl.when(peer < me)
        def _():
            pl.semaphore_signal(ready.at[me], inc=1, device_id=at(peer), device_id_type=MESH)

    mine_in = (
        pltpu.make_async_copy(items_ref, iall.at[0], in_sem.at[0]),
        pltpu.make_async_copy(users_ref, uall.at[me], in_sem.at[1]),
        pltpu.make_async_copy(pos_ref, pall.at[me], in_sem.at[2]),
    )
    each(greet)
    pl.semaphore_signal(barrier, inc=1, device_id=to_twin, device_id_type=MESH)

    @pl.when(batch == 0)
    def _():
        pl.semaphore_signal(barrier, inc=1, device_id=to_other, device_id_type=MESH)

    for copy in mine_in:
        copy.start()
    pl.semaphore_wait(barrier, me + batch + 1)
    each(answer)

    @pl.when(batch == 1)
    def _():
        pl.semaphore_signal(x_ready.at[0], inc=1, device_id=to_other, device_id_type=MESH)

    for copy in mine_in:
        copy.wait()

    def users_copy(step, source):
        return remote(uall.at[me], uall.at[source], u_ss.at[step], u_rs.at[source], at(peer_at(step)))

    def pos_copy(step, source):
        return remote(pall.at[me], pall.at[source], p_ss.at[step], p_rs.at[source], at(peer_at(step)))

    def stat_copy(step, source):
        return remote(stat, stat_all.at[source], s_ss.at[step], s_rs.at[source], at(peer_at(step)))

    half = peers // 2
    side = me // half
    place = lax.rem(me, half)

    def near_at(step):
        return side * half + lax.rem(place + step, half)

    def far_at(step):
        return (1 - side) * half + lax.rem(place + step, half)

    def near_copy(step, source):
        return to_near(near_at(step), source)

    def far_copy(step, source):
        return to_far(far_at(step), source)

    def to_near(peer, source):
        return remote(term.at[peer], near_recv.at[source], g_ss.at[peer], g_rs.at[source], at(peer))

    def to_far(peer, source):
        return remote(ug_send.at[peer], far_recv.at[source], g_ss.at[peer], g_rs.at[source], at(peer))

    half_rows = per // PARTS

    def items_copy(source, slot, p, device):
        block = pl.ds(p * half_rows, half_rows)
        return remote(
            iall.at[source, block], iall.at[slot, block], i_ss.at[slot, p], i_rs.at[slot, p], device
        )

    from_other = [items_copy(0, 2, p, to_other) for p in range(PARTS)]
    from_twin = [items_copy(0, 1, p, to_twin) for p in range(PARTS)]
    from_diag = [items_copy(2, 3, p, to_twin) for p in range(PARTS)]

    def low_first(body):
        if peers <= 8:
            for peer in range(peers):
                body(peer)
        else:
            pl.loop(0, peers)(body)

    def send_down(peer):
        step = lax.rem(peer - me + peers, peers)

        @pl.when(peer < me)
        def _():
            pos_copy(step, me).start()
            users_copy(step, me).start()

    def send_up(step):
        peer = peer_at(step)

        @pl.when(peer > me)
        def _():
            pl.semaphore_wait(ready.at[peer], 1)
            pos_copy(step, me).start()
            users_copy(step, me).start()

    @pl.when(batch == 1)
    def _():
        for copy in from_other:
            copy.start()

    low_first(send_down)
    for copy in from_twin:
        copy.start()

    @pl.when(batch == 0)
    def _():
        pl.semaphore_wait(x_ready.at[0], 1)
        for copy in from_other:
            copy.start()

    rising(send_up)
    for p in range(PARTS):
        from_other[p].wait_recv()
        from_diag[p].start()
    def near_in(step):
        source = near_at(step)
        users_copy(step, source).wait_recv()
        pos_copy(step, source).wait_recv()

    def far_in(step):
        source = far_at(step)
        users_copy(step, source).wait_recv()
        pos_copy(step, source).wait_recv()

    def mate_copy(src, ids, k, p, part, device):
        block = pl.ds(part * half, half)
        return (
            remote(ids.at[block], mate_ids.at[k, block], n_ss.at[k, p], n_rs.at[k, p], device),
            remote(src.at[block], mates.at[k, block], m_ss.at[k, p], m_rs.at[k, p], device),
        )

    halves = (side, 1 - side)
    to_mates = [
        [mate_copy(uall, pall, 1, p, halves[p], to_other) for p in range(2)],
        [mate_copy(uall, pall, 0, p, halves[p], to_twin) for p in range(2)],
    ]
    onward = [mate_copy(mates.at[1], mate_ids.at[1], 2, p, halves[p], to_twin) for p in range(2)]

    def lend(p):
        for pair in to_mates:
            for copy in pair[p]:
                copy.start()

    steps(half, 1, near_in)
    lend(0)

    def over_chunks(body):
        if chunks <= 2:
            for chunk in range(chunks):
                body(chunk)
        else:
            pl.loop(0, chunks)(body)

    def over_half(which, body):
        count = chunks // 2
        if count == 1:
            body(which)
        else:
            pl.loop(0, count)(lambda chunk: body(which * count + chunk))

    homes = (
        batch * total_index + index,
        batch * total_index + twin,
        other * total_index + index,
        other * total_index + twin,
    )
    row = lax.broadcasted_iota(jnp.int32, (per, slots * own), 0)

    def lane_ids(ids, chunk):
        return jnp.concatenate([ids[chunk * slots + k] for k in range(slots)], axis=1)

    def ids_of(chunk):
        return lane_ids(pall, chunk)

    def joined(blocks, chunk):
        return jnp.concatenate(
            [blocks[chunk * slots + k].astype(F32) for k in range(slots)], axis=0
        ).astype(BF16)

    def prepare(chunk):
        ucat[chunk] = joined(uall, chunk)

    def meet(k, chunk):
        mate_cat[k, chunk] = joined(mates.at[k], chunk)
        mate_logit[k, chunk] = lax.dot_general(
            iall[0], mate_cat[k, chunk], NT, preferred_element_type=F32
        )

    def folded(combine, block):
        return combine(block.reshape(block.shape[0] // 8, 8, block.shape[1]), axis=0)

    def forward(chunk):
        logits = [
            lax.dot_general(iall[q], ucat[chunk], NT, preferred_element_type=F32)
            for q in range(QUAD)
        ]
        tops = [folded(jnp.max, logit) for logit in logits]
        top = jnp.max(functools.reduce(jnp.maximum, tops), axis=0, keepdims=True)
        total = jnp.zeros_like(tops[0])
        for q in range(QUAD):
            e = jnp.exp(logits[q] - top)
            e_ref[chunk, q * per : (q + 1) * per] = e.astype(BF16)
            total = total + folded(jnp.sum, e)
        stat[chunk] = top + jnp.log(jnp.sum(total, axis=0, keepdims=True))
        top_ref[chunk] = top
        logit_ref[chunk] = logits[0]

    for copy in from_twin + from_diag:
        copy.wait_recv()

    def advance(chunk):
        prepare(chunk)
        forward(chunk)

    over_half(side, advance)
    steps(half, 0, far_in)
    over_half(1 - side, advance)
    def tell(peer):
        @pl.when(peer != me)
        def _():
            stat_copy(lax.rem(peer - me + peers, peers), me).start()

    low_first(tell)
    stat_all[me] = stat[...]
    lend(1)

    def mate_in(k, p):
        for copy in mate_copy(uall, pall, k, p, halves[p], to_twin):
            copy.wait_recv()

    def columns(rows):
        return jnp.transpose(jnp.concatenate([rows] * (8 // rows.shape[0]), axis=0))

    def gather_terms(chunk):
        mix = jnp.zeros((slots * own, ucat.shape[2]), F32)
        pick = jnp.zeros((slots * own, ucat.shape[2]), F32)
        for q in range(QUAD):
            here = row == ids_of(chunk) - homes[q] * per
            hit = jnp.where(here, 1.0, 0.0).astype(BF16)
            rest = jnp.where(here, 0.0, e_ref[chunk, q * per : (q + 1) * per].astype(F32)).astype(BF16)
            part = lax.dot_general(rest, iall[q], TN, preferred_element_type=F32)
            mix = mix + part
            pick = pick + lax.dot_general(hit, iall[q], TN, preferred_element_type=F32)
        blend[chunk] = mix
        picked[chunk] = pick
        pos[chunk] = lax.dot_general(
            jnp.ones((8, pick.shape[1]), F32), ucat[chunk].astype(F32) * pick, NT,
            precision=lax.Precision.HIGHEST, preferred_element_type=F32,
        )[0:1]

    def pos_out(step, source):
        return remote(pos, pos_all.at[source], h_ss.at[step], h_rs.at[source], at(peer_at(step)))

    over_chunks(gather_terms)
    each(lambda step: pos_out(step, me).start())
    pos_all[me] = pos[...]
    for p in range(2):
        mate_in(0, p)
    over_chunks(functools.partial(meet, 0))
    mate_in(1, 0)
    for copy in onward[0]:
        copy.start()
    for copy in from_other + from_twin + from_diag:
        copy.wait_send()
    for copy in (users_copy, pos_copy):
        each(lambda step: copy(step, me).wait_send())
    each(lambda step: stat_copy(step, peer_at(step)).wait_recv())


    def rescale(chunk):
        lses = stat_all[:, chunk]
        peak = jnp.max(lses, axis=0)
        lse_ref[chunk] = peak + jnp.log(jnp.sum(jnp.exp(lses - peak[None]), axis=0))

    def user_terms(chunk):
        lse = lse_ref[chunk]
        at_pos = jnp.exp(jnp.minimum(pos[chunk] - lse, 0.0)) - 1.0
        at_top = jnp.exp(top_ref[chunk] - lse)
        scale = columns(jnp.concatenate([at_top, at_pos], axis=0).astype(BF16).astype(F32))
        grad = blend[chunk] * scale[:, 0:1] + picked[chunk] * scale[:, 1:2]
        for k in range(slots):
            part = grad[k * own : (k + 1) * own]
            term[chunk * slots + k] = part
            ug_send[chunk * slots + k] = part.astype(BF16)

    def own_term(chunk):
        hit = row == ids_of(chunk) - homes[0] * per
        w = jnp.exp(logit_ref[chunk] - lse_ref[chunk]) - jnp.where(hit, 1.0, 0.0)
        return jnp.dot(w.astype(BF16), ucat[chunk], preferred_element_type=F32)

    def mate_term(k, chunk):
        hit = row == lane_ids(mate_ids.at[k], chunk) - homes[0] * per
        w = jnp.exp(mate_logit[k, chunk] - mate_lse[k, chunk]) - jnp.where(hit, 1.0, 0.0)
        return jnp.dot(w.astype(BF16), mate_cat[k, chunk], preferred_element_type=F32)

    def total_of(one):
        if chunks == 2:
            return one(0) + one(1)
        return lax.fori_loop(1, chunks, lambda chunk, acc: acc + one(chunk), one(0))

    lse_copies = [
        remote(lse_ref, mate_lse.at[k], l_ss.at[k], l_rs.at[k], device)
        for k, device in enumerate((to_twin, to_other, to_diag))
    ]

    over_chunks(rescale)
    for copy in (lse_copies[1], lse_copies[2], lse_copies[0]):
        copy.start()
    over_chunks(user_terms)
    def give(peer):
        @pl.when(peer // half != side)
        def _():
            to_far(peer, me).start()

        @pl.when(jnp.logical_and(peer // half == side, peer != me))
        def _():
            to_near(peer, me).start()

    low_first(give)
    ig_ref[...] = total_of(own_term)
    mate_in(1, 1)
    for copy in onward[1]:
        copy.start()
    over_chunks(functools.partial(meet, 1))
    for p in range(2):
        mate_in(2, p)
    over_chunks(functools.partial(meet, 2))
    each(lambda step: stat_copy(step, me).wait_send())
    each(lambda step: pos_out(step, me).wait_send())
    for p in range(2):
        for copy in (*to_mates[0][p], *to_mates[1][p], *onward[p]):
            copy.wait_send()
    for copy in lse_copies:
        copy.wait_send()
    for k in (0, 2, 1):
        lse_copies[k].wait_recv()
        ig_ref[...] += total_of(functools.partial(mate_term, k))

    each(lambda step: pos_out(step, peer_at(step)).wait_recv())
    losses = lse_ref[me // slots] - jnp.sum(pos_all[:, me // slots], axis=0)
    loss = jnp.zeros((1, own), F32)
    for k in range(slots):
        loss = jnp.where(lax.rem(me, slots) == k, losses[:, k * own : (k + 1) * own], loss)
    loss_ref[...] = loss

    ug_ref[...] = term[me]

    def gather_near(step):
        near_copy(step, near_at(step)).wait_recv()
        ug_ref[...] += near_recv[near_at(step)]

    def gather_far(step):
        far_copy(step, far_at(step)).wait_recv()
        ug_ref[...] += far_recv[far_at(step)].astype(F32)

    steps(half, 1, gather_near)
    steps(half, 0, gather_far)
    steps(half, 0, lambda step: far_copy(step, me).wait_send())
    steps(half, 1, lambda step: near_copy(step, me).wait_send())


def settle(loss_in, ug_in, ig_in, loss_out, ug_out, ig_out, sems):
    copies = [
        pltpu.make_async_copy(src, dst, sems.at[k])
        for k, (src, dst) in enumerate(((ig_in, ig_out), (ug_in, ug_out), (loss_in, loss_out)))
    ]
    for copy in copies:
        copy.start()
    for copy in copies:
        copy.wait()


def local(users, items, pos_ids):
    own, width = users.shape
    per = items.shape[0]
    peers = lax.axis_size("items") // 2
    slots = math.gcd(peers // 2, 4)
    chunks = peers // slots
    lanes = slots * own
    dma = pltpu.SemaphoreType.DMA
    vmem = pl.BlockSpec(memory_space=pltpu.VMEM)
    hbm = pl.BlockSpec(memory_space=pltpu.HBM)
    loss, user_grad, item_grad = pl.pallas_call(
        functools.partial(kernel, peers, slots),
        out_shape=(
            pltpu.VMEM((1, own), F32),
            pltpu.VMEM((own, width), F32),
            pltpu.VMEM((per, width), F32),
        ),
        in_specs=[hbm] * 3,
        out_specs=(vmem, vmem, vmem),
        scratch_shapes=[
            pltpu.VMEM((peers, own, width), BF16),
            pltpu.VMEM((peers, 1, own), jnp.int32),
            pltpu.VMEM((QUAD, per, width), BF16),
            pltpu.VMEM((chunks, lanes, width), BF16),
            pltpu.VMEM((chunks, QUAD * per, lanes), BF16),
            pltpu.VMEM((chunks, per, lanes), F32),
            pltpu.VMEM((chunks, lanes, width), F32),
            pltpu.VMEM((chunks, lanes, width), F32),
            pltpu.VMEM((chunks, 1, lanes), F32),
            pltpu.VMEM((chunks, 1, lanes), F32),
            pltpu.VMEM((peers, chunks, 1, lanes), F32),
            pltpu.VMEM((chunks, 1, lanes), F32),
            pltpu.VMEM((peers, chunks, 1, lanes), F32),
            pltpu.VMEM((peers, own, width), F32),
            pltpu.VMEM((peers, own, width), BF16),
            pltpu.VMEM((peers, own, width), F32),
            pltpu.VMEM((peers, own, width), BF16),
            pltpu.VMEM((3, peers, own, width), BF16),
            pltpu.VMEM((3, peers, 1, own), jnp.int32),
            pltpu.VMEM((3, chunks, lanes, width), BF16),
            pltpu.VMEM((3, chunks, per, lanes), F32),
            pltpu.VMEM((chunks, 1, lanes), F32),
            pltpu.VMEM((3, chunks, 1, lanes), F32),
            dma((peers,)), dma((peers,)),
            dma((peers,)), dma((peers,)),
            dma((QUAD, PARTS)), dma((QUAD, PARTS)),
            dma((peers,)), dma((peers,)),
            dma((peers,)), dma((peers,)),
            dma((peers,)), dma((peers,)),
            dma((3, 2)), dma((3, 2)),
            dma((3, 2)), dma((3, 2)),
            dma((3,)), dma((3,)),
            dma((3,)),
            pltpu.SemaphoreType.REGULAR((peers,)),
            pltpu.SemaphoreType.REGULAR((1,)),
        ],
        compiler_params=pltpu.CompilerParams(
            collective_id=0, has_side_effects=True, vmem_limit_bytes=56 * 1024 * 1024
        ),
    )(*(pltpu.with_memory_space_constraint(v, pltpu.HBM) for v in (users, items, pos_ids.reshape(1, own))))
    loss, user_grad, item_grad = pl.pallas_call(
        settle,
        out_shape=(
            jax.ShapeDtypeStruct((1, own), F32),
            jax.ShapeDtypeStruct((own, width), F32),
            jax.ShapeDtypeStruct((per, width), F32),
        ),
        in_specs=[vmem] * 3,
        out_specs=(hbm,) * 3,
        scratch_shapes=[dma((3,))],
        compiler_params=pltpu.CompilerParams(vmem_limit_bytes=4 * 1024 * 1024),
    )(loss, user_grad, item_grad)
    return loss.reshape(own), user_grad, item_grad


def solution(mesh):
    placed = (P(("batch", "items"), None), P(("batch", "items"), None), P(("batch", "items")))
    return jax.shard_map(
        local,
        mesh=mesh,
        in_specs=placed,
        out_specs=(P(("batch", "items")), P(("batch", "items"), None), P(("batch", "items"), None)),
        check_vma=False,
    )
```

```python
import functools
import math

import jax
import jax.numpy as jnp
from jax import lax
from jax.experimental import pallas as pl
from jax.experimental.pallas import tpu as pltpu
from jax.sharding import PartitionSpec as P

F32 = jnp.float32
BF16 = jnp.bfloat16
MESH = pl.DeviceIdType.MESH
NT = (((1,), (1,)), ((), ()))
TN = (((0,), (0,)), ((), ()))
QUAD = 4
PARTS = 2


def kernel(
    peers, slots, users_ref, items_ref, pos_ref,
    loss_ref, ug_ref, ig_ref,
    uall, pall, iall, ucat, e_ref, logit_ref, blend, picked, top_ref, stat, stat_all, pos, pos_all,
    term, ug_send, near_recv, far_recv, mates, mate_ids, mate_cat, mate_logit, lse_ref, mate_lse,
    u_ss, u_rs, p_ss, p_rs, i_ss, i_rs, s_ss, s_rs, h_ss, h_rs, g_ss, g_rs, m_ss, m_rs, n_ss, n_rs, l_ss, l_rs,
    in_sem, ready, x_ready,
):
    own = users_ref.shape[0]
    per = items_ref.shape[0]
    chunks = peers // slots
    batch = lax.axis_index("batch")
    index = lax.axis_index("items")
    core = lax.rem(index, 2)
    me = index // 2
    twin = index + 1 - 2 * core
    other = 1 - batch
    total_index = 2 * peers

    def at(peer):
        return {"batch": batch, "items": 2 * peer + core}

    def peer_at(step):
        return lax.rem(me + step, peers)

    to_twin = {"batch": batch, "items": twin}
    to_other = {"batch": other, "items": index}
    to_diag = {"batch": other, "items": twin}

    def remote(src, dst, ss, rs, device):
        return pltpu.make_async_remote_copy(
            src_ref=src, dst_ref=dst, send_sem=ss, recv_sem=rs, device_id=device, device_id_type=MESH
        )

    barrier = pltpu.get_barrier_semaphore()

    def steps(count, first, body):
        if count <= 8:
            for step in range(count - 1, first - 1, -1):
                body(step)
        else:
            pl.loop(first, count)(body)

    def each(body):
        steps(peers, 1, body)

    def rising(body):
        if peers <= 8:
            for step in range(1, peers):
                body(step)
        else:
            pl.loop(1, peers)(body)

    def greet(step):
        peer = peer_at(step)

        @pl.when(peer > me)
        def _():
            pl.semaphore_signal(barrier, inc=1, device_id=at(peer), device_id_type=MESH)

    def answer(step):
        peer = peer_at(step)

        @pl.when(peer < me)
        def _():
            pl.semaphore_signal(ready.at[me], inc=1, device_id=at(peer), device_id_type=MESH)

    mine_in = (
        pltpu.make_async_copy(items_ref, iall.at[0], in_sem.at[0]),
        pltpu.make_async_copy(users_ref, uall.at[me], in_sem.at[1]),
        pltpu.make_async_copy(pos_ref, pall.at[me], in_sem.at[2]),
    )
    each(greet)
    pl.semaphore_signal(barrier, inc=1, device_id=to_twin, device_id_type=MESH)

    @pl.when(batch == 0)
    def _():
        pl.semaphore_signal(barrier, inc=1, device_id=to_other, device_id_type=MESH)

    for copy in mine_in:
        copy.start()
    pl.semaphore_wait(barrier, me + batch + 1)
    each(answer)

    @pl.when(batch == 1)
    def _():
        pl.semaphore_signal(x_ready.at[0], inc=1, device_id=to_other, device_id_type=MESH)

    for copy in mine_in:
        copy.wait()

    def users_copy(step, source):
        return remote(uall.at[me], uall.at[source], u_ss.at[step], u_rs.at[source], at(peer_at(step)))

    def pos_copy(step, source):
        return remote(pall.at[me], pall.at[source], p_ss.at[step], p_rs.at[source], at(peer_at(step)))

    def stat_copy(step, source):
        return remote(stat, stat_all.at[source], s_ss.at[step], s_rs.at[source], at(peer_at(step)))

    half = peers // 2
    side = me // half
    place = lax.rem(me, half)

    def near_at(step):
        return side * half + lax.rem(place + step, half)

    def far_at(step):
        return (1 - side) * half + lax.rem(place + step, half)

    def near_copy(step, source):
        return to_near(near_at(step), source)

    def far_copy(step, source):
        return to_far(far_at(step), source)

    def to_near(peer, source):
        return remote(term.at[peer], near_recv.at[source], g_ss.at[peer], g_rs.at[source], at(peer))

    def to_far(peer, source):
        return remote(ug_send.at[peer], far_recv.at[source], g_ss.at[peer], g_rs.at[source], at(peer))

    half_rows = per // PARTS

    def items_copy(source, slot, p, device):
        block = pl.ds(p * half_rows, half_rows)
        return remote(
            iall.at[source, block], iall.at[slot, block], i_ss.at[slot, p], i_rs.at[slot, p], device
        )

    from_other = [items_copy(0, 2, p, to_other) for p in range(PARTS)]
    from_twin = [items_copy(0, 1, p, to_twin) for p in range(PARTS)]
    from_diag = [items_copy(2, 3, p, to_twin) for p in range(PARTS)]

    def low_first(body):
        if peers <= 8:
            for peer in range(peers):
                body(peer)
        else:
            pl.loop(0, peers)(body)

    def send_down(peer):
        step = lax.rem(peer - me + peers, peers)

        @pl.when(peer < me)
        def _():
            users_copy(step, me).start()
            pos_copy(step, me).start()

    def send_up(step):
        peer = peer_at(step)

        @pl.when(peer > me)
        def _():
            pl.semaphore_wait(ready.at[peer], 1)
            users_copy(step, me).start()
            pos_copy(step, me).start()

    @pl.when(batch == 1)
    def _():
        for copy in from_other:
            copy.start()

    low_first(send_down)
    for copy in from_twin:
        copy.start()

    @pl.when(batch == 0)
    def _():
        pl.semaphore_wait(x_ready.at[0], 1)
        for copy in from_other:
            copy.start()

    rising(send_up)
    for p in range(PARTS):
        from_other[p].wait_recv()
        from_diag[p].start()
    def near_in(step):
        source = near_at(step)
        users_copy(step, source).wait_recv()

    def far_in(step):
        source = far_at(step)
        users_copy(step, source).wait_recv()

    def mate_copy(src, k, p, part, device):
        block = pl.ds(part * half, half)
        return remote(src.at[block], mates.at[k, block], m_ss.at[k, p], m_rs.at[k, p], device)

    def ids_copy(src, k, device):
        return remote(src, mate_ids.at[k], n_ss.at[k], n_rs.at[k], device)

    ids_to_mates = (ids_copy(pall, 1, to_other), ids_copy(pall, 0, to_twin))
    ids_onward = ids_copy(mate_ids.at[1], 2, to_twin)

    halves = (side, 1 - side)
    to_mates = [
        [mate_copy(uall, 1, p, halves[p], to_other) for p in range(2)],
        [mate_copy(uall, 0, p, halves[p], to_twin) for p in range(2)],
    ]
    onward = [mate_copy(mates.at[1], 2, p, halves[p], to_twin) for p in range(2)]

    def lend(p):
        for pair in to_mates:
            pair[p].start()

    steps(half, 1, near_in)
    lend(0)

    def over_chunks(body):
        if chunks <= 2:
            for chunk in range(chunks):
                body(chunk)
        else:
            pl.loop(0, chunks)(body)

    def over_half(which, body):
        count = chunks // 2
        if count == 1:
            body(which)
        else:
            pl.loop(0, count)(lambda chunk: body(which * count + chunk))

    homes = (
        batch * total_index + index,
        batch * total_index + twin,
        other * total_index + index,
        other * total_index + twin,
    )
    row = lax.broadcasted_iota(jnp.int32, (per, slots * own), 0)

    def lane_ids(ids, chunk):
        return jnp.concatenate([ids[chunk * slots + k] for k in range(slots)], axis=1)

    def ids_of(chunk):
        return lane_ids(pall, chunk)

    def joined(blocks, chunk):
        return jnp.concatenate(
            [blocks[chunk * slots + k].astype(F32) for k in range(slots)], axis=0
        ).astype(BF16)

    def prepare(chunk):
        ucat[chunk] = joined(uall, chunk)

    def meet(k, chunk):
        mate_cat[k, chunk] = joined(mates.at[k], chunk)
        mate_logit[k, chunk] = lax.dot_general(
            iall[0], mate_cat[k, chunk], NT, preferred_element_type=F32
        )

    def folded(combine, block):
        return combine(block.reshape(block.shape[0] // 8, 8, block.shape[1]), axis=0)

    def forward(chunk):
        logits = [
            lax.dot_general(iall[q], ucat[chunk], NT, preferred_element_type=F32)
            for q in range(QUAD)
        ]
        tops = [folded(jnp.max, logit) for logit in logits]
        top = jnp.max(functools.reduce(jnp.maximum, tops), axis=0, keepdims=True)
        total = jnp.zeros_like(tops[0])
        for q in range(QUAD):
            e = jnp.exp(logits[q] - top)
            e_ref[chunk, q * per : (q + 1) * per] = e.astype(BF16)
            total = total + folded(jnp.sum, e)
        stat[chunk] = top + jnp.log(jnp.sum(total, axis=0, keepdims=True))
        top_ref[chunk] = top
        logit_ref[chunk] = logits[0]

    for copy in from_twin + from_diag:
        copy.wait_recv()

    def advance(chunk):
        prepare(chunk)
        forward(chunk)

    over_half(side, advance)
    steps(half, 0, far_in)
    over_half(1 - side, advance)
    def tell(peer):
        @pl.when(peer != me)
        def _():
            stat_copy(lax.rem(peer - me + peers, peers), me).start()

    low_first(tell)
    stat_all[me] = stat[...]
    lend(1)
    each(lambda step: pos_copy(step, peer_at(step)).wait_recv())
    for copy in ids_to_mates:
        copy.start()

    def mate_in(k, p):
        mate_copy(uall, k, p, halves[p], to_twin).wait_recv()

    def columns(rows):
        return jnp.transpose(jnp.concatenate([rows] * (8 // rows.shape[0]), axis=0))

    def gather_terms(chunk):
        mix = jnp.zeros((slots * own, ucat.shape[2]), F32)
        pick = jnp.zeros((slots * own, ucat.shape[2]), F32)
        for q in range(QUAD):
            here = row == ids_of(chunk) - homes[q] * per
            hit = jnp.where(here, 1.0, 0.0).astype(BF16)
            rest = jnp.where(here, 0.0, e_ref[chunk, q * per : (q + 1) * per].astype(F32)).astype(BF16)
            part = lax.dot_general(rest, iall[q], TN, preferred_element_type=F32)
            mix = mix + part
            pick = pick + lax.dot_general(hit, iall[q], TN, preferred_element_type=F32)
        blend[chunk] = mix
        picked[chunk] = pick
        pos[chunk] = lax.dot_general(
            jnp.ones((8, pick.shape[1]), F32), ucat[chunk].astype(F32) * pick, NT,
            precision=lax.Precision.HIGHEST, preferred_element_type=F32,
        )[0:1]

    def pos_out(step, source):
        return remote(pos, pos_all.at[source], h_ss.at[step], h_rs.at[source], at(peer_at(step)))

    over_chunks(gather_terms)
    each(lambda step: pos_out(step, me).start())
    pos_all[me] = pos[...]
    for p in range(2):
        mate_in(0, p)
    over_chunks(functools.partial(meet, 0))
    mate_in(1, 0)
    onward[0].start()
    for copy in from_other + from_twin + from_diag:
        copy.wait_send()
    for copy in (users_copy, pos_copy):
        each(lambda step: copy(step, me).wait_send())
    each(lambda step: stat_copy(step, peer_at(step)).wait_recv())


    def rescale(chunk):
        lses = stat_all[:, chunk]
        peak = jnp.max(lses, axis=0)
        lse_ref[chunk] = peak + jnp.log(jnp.sum(jnp.exp(lses - peak[None]), axis=0))

    def user_terms(chunk):
        lse = lse_ref[chunk]
        at_pos = jnp.exp(jnp.minimum(pos[chunk] - lse, 0.0)) - 1.0
        at_top = jnp.exp(top_ref[chunk] - lse)
        scale = columns(jnp.concatenate([at_top, at_pos], axis=0).astype(BF16).astype(F32))
        grad = blend[chunk] * scale[:, 0:1] + picked[chunk] * scale[:, 1:2]
        for k in range(slots):
            part = grad[k * own : (k + 1) * own]
            term[chunk * slots + k] = part
            ug_send[chunk * slots + k] = part.astype(BF16)

    def own_term(chunk):
        hit = row == ids_of(chunk) - homes[0] * per
        w = jnp.exp(logit_ref[chunk] - lse_ref[chunk]) - jnp.where(hit, 1.0, 0.0)
        return jnp.dot(w.astype(BF16), ucat[chunk], preferred_element_type=F32)

    def mate_term(k, chunk):
        hit = row == lane_ids(mate_ids.at[k], chunk) - homes[0] * per
        w = jnp.exp(mate_logit[k, chunk] - mate_lse[k, chunk]) - jnp.where(hit, 1.0, 0.0)
        return jnp.dot(w.astype(BF16), mate_cat[k, chunk], preferred_element_type=F32)

    def total_of(one):
        if chunks == 2:
            return one(0) + one(1)
        return lax.fori_loop(1, chunks, lambda chunk, acc: acc + one(chunk), one(0))

    lse_copies = [
        remote(lse_ref, mate_lse.at[k], l_ss.at[k], l_rs.at[k], device)
        for k, device in enumerate((to_twin, to_other, to_diag))
    ]

    def give(peer):
        @pl.when(peer // half != side)
        def _():
            to_far(peer, me).start()

        @pl.when(jnp.logical_and(peer // half == side, peer != me))
        def _():
            to_near(peer, me).start()

    def send_terms(chunk):
        user_terms(chunk)
        if chunks <= 2:
            for k in range(slots):
                give(chunk * slots + k)
        else:
            pl.loop(0, slots)(lambda k: give(chunk * slots + k))

    def send_lses():
        for copy in (lse_copies[1], lse_copies[2], lse_copies[0]):
            copy.start()

    if chunks <= 2:
        rescale(0)
        send_terms(0)
        for chunk in range(1, chunks):
            rescale(chunk)
        send_lses()
        for chunk in range(1, chunks):
            send_terms(chunk)
    else:
        over_chunks(rescale)
        send_lses()
        over_chunks(send_terms)
    ig_ref[...] = total_of(own_term)
    mate_in(1, 1)
    onward[1].start()
    ids_to_mates[0].wait_recv()
    ids_onward.start()
    over_chunks(functools.partial(meet, 1))
    for p in range(2):
        mate_in(2, p)
    over_chunks(functools.partial(meet, 2))
    each(lambda step: stat_copy(step, me).wait_send())
    each(lambda step: pos_out(step, me).wait_send())
    for p in range(2):
        for copy in (to_mates[0][p], to_mates[1][p], onward[p]):
            copy.wait_send()
    for copy in (*ids_to_mates, ids_onward):
        copy.wait_send()
    ids_to_mates[1].wait_recv()
    ids_onward.wait_recv()
    for copy in lse_copies:
        copy.wait_send()
    for k in (0, 2, 1):
        lse_copies[k].wait_recv()
        ig_ref[...] += total_of(functools.partial(mate_term, k))

    each(lambda step: pos_out(step, peer_at(step)).wait_recv())
    losses = lse_ref[me // slots] - jnp.sum(pos_all[:, me // slots], axis=0)
    loss = jnp.zeros((1, own), F32)
    for k in range(slots):
        loss = jnp.where(lax.rem(me, slots) == k, losses[:, k * own : (k + 1) * own], loss)
    loss_ref[...] = loss

    ug_ref[...] = term[me]

    def gather_near(step):
        near_copy(step, near_at(step)).wait_recv()
        ug_ref[...] += near_recv[near_at(step)]

    def gather_far(step):
        far_copy(step, far_at(step)).wait_recv()
        ug_ref[...] += far_recv[far_at(step)].astype(F32)

    steps(half, 0, lambda step: far_copy(step, me).wait_send())
    steps(half, 1, lambda step: near_copy(step, me).wait_send())
    steps(half, 1, gather_near)
    steps(half, 0, gather_far)


def settle(loss_in, ug_in, ig_in, loss_out, ug_out, ig_out, sems):
    copies = [
        pltpu.make_async_copy(src, dst, sems.at[k])
        for k, (src, dst) in enumerate(((ig_in, ig_out), (ug_in, ug_out), (loss_in, loss_out)))
    ]
    for copy in copies:
        copy.start()
    for copy in copies:
        copy.wait()


def local(users, items, pos_ids):
    own, width = users.shape
    per = items.shape[0]
    peers = lax.axis_size("items") // 2
    slots = math.gcd(peers // 2, 4)
    chunks = peers // slots
    lanes = slots * own
    dma = pltpu.SemaphoreType.DMA
    vmem = pl.BlockSpec(memory_space=pltpu.VMEM)
    hbm = pl.BlockSpec(memory_space=pltpu.HBM)
    loss, user_grad, item_grad = pl.pallas_call(
        functools.partial(kernel, peers, slots),
        out_shape=(
            pltpu.VMEM((1, own), F32),
            pltpu.VMEM((own, width), F32),
            pltpu.VMEM((per, width), F32),
        ),
        in_specs=[hbm] * 3,
        out_specs=(vmem, vmem, vmem),
        scratch_shapes=[
            pltpu.VMEM((peers, own, width), BF16),
            pltpu.VMEM((peers, 1, own), jnp.int32),
            pltpu.VMEM((QUAD, per, width), BF16),
            pltpu.VMEM((chunks, lanes, width), BF16),
            pltpu.VMEM((chunks, QUAD * per, lanes), BF16),
            pltpu.VMEM((chunks, per, lanes), F32),
            pltpu.VMEM((chunks, lanes, width), F32),
            pltpu.VMEM((chunks, lanes, width), F32),
            pltpu.VMEM((chunks, 1, lanes), F32),
            pltpu.VMEM((chunks, 1, lanes), F32),
            pltpu.VMEM((peers, chunks, 1, lanes), F32),
            pltpu.VMEM((chunks, 1, lanes), F32),
            pltpu.VMEM((peers, chunks, 1, lanes), F32),
            pltpu.VMEM((peers, own, width), F32),
            pltpu.VMEM((peers, own, width), BF16),
            pltpu.VMEM((peers, own, width), F32),
            pltpu.VMEM((peers, own, width), BF16),
            pltpu.VMEM((3, peers, own, width), BF16),
            pltpu.VMEM((3, peers, 1, own), jnp.int32),
            pltpu.VMEM((3, chunks, lanes, width), BF16),
            pltpu.VMEM((3, chunks, per, lanes), F32),
            pltpu.VMEM((chunks, 1, lanes), F32),
            pltpu.VMEM((3, chunks, 1, lanes), F32),
            dma((peers,)), dma((peers,)),
            dma((peers,)), dma((peers,)),
            dma((QUAD, PARTS)), dma((QUAD, PARTS)),
            dma((peers,)), dma((peers,)),
            dma((peers,)), dma((peers,)),
            dma((peers,)), dma((peers,)),
            dma((3, 2)), dma((3, 2)),
            dma((3,)), dma((3,)),
            dma((3,)), dma((3,)),
            dma((3,)),
            pltpu.SemaphoreType.REGULAR((peers,)),
            pltpu.SemaphoreType.REGULAR((1,)),
        ],
        compiler_params=pltpu.CompilerParams(
            collective_id=0, has_side_effects=True, vmem_limit_bytes=56 * 1024 * 1024
        ),
    )(*(pltpu.with_memory_space_constraint(v, pltpu.HBM) for v in (users, items, pos_ids.reshape(1, own))))
    loss, user_grad, item_grad = pl.pallas_call(
        settle,
        out_shape=(
            jax.ShapeDtypeStruct((1, own), F32),
            jax.ShapeDtypeStruct((own, width), F32),
            jax.ShapeDtypeStruct((per, width), F32),
        ),
        in_specs=[vmem] * 3,
        out_specs=(hbm,) * 3,
        scratch_shapes=[dma((3,))],
        compiler_params=pltpu.CompilerParams(vmem_limit_bytes=4 * 1024 * 1024),
    )(loss, user_grad, item_grad)
    return loss.reshape(own), user_grad, item_grad


def solution(mesh):
    placed = (P(("batch", "items"), None), P(("batch", "items"), None), P(("batch", "items")))
    return jax.shard_map(
        local,
        mesh=mesh,
        in_specs=placed,
        out_specs=(P(("batch", "items")), P(("batch", "items"), None), P(("batch", "items"), None)),
        check_vma=False,
    )
```

```python
import functools
import math

import jax
import jax.numpy as jnp
from jax import lax
from jax.experimental import pallas as pl
from jax.experimental.pallas import tpu as pltpu
from jax.sharding import PartitionSpec as P

F32 = jnp.float32
BF16 = jnp.bfloat16
MESH = pl.DeviceIdType.MESH
NT = (((1,), (1,)), ((), ()))
TN = (((0,), (0,)), ((), ()))
QUAD = 4
PARTS = 2


def kernel(
    peers, slots, users_ref, items_ref, pos_ref,
    loss_ref, ug_ref, ig_ref,
    uall, pall, iall, ucat, e_ref, logit_ref, blend, picked, top_ref, stat, stat_all, pos, pos_all,
    term, ug_send, near_recv, far_recv, mates, mate_ids, mate_cat, mate_logit, lse_ref, mate_lse,
    u_ss, u_rs, p_ss, p_rs, i_ss, i_rs, s_ss, s_rs, h_ss, h_rs, g_ss, g_rs, m_ss, m_rs, n_ss, n_rs, l_ss, l_rs,
    in_sem, ready, x_ready,
):
    own = users_ref.shape[0]
    per = items_ref.shape[0]
    chunks = peers // slots
    batch = lax.axis_index("batch")
    index = lax.axis_index("items")
    core = lax.rem(index, 2)
    me = index // 2
    twin = index + 1 - 2 * core
    other = 1 - batch
    total_index = 2 * peers

    def at(peer):
        return {"batch": batch, "items": 2 * peer + core}

    def peer_at(step):
        return lax.rem(me + step, peers)

    to_twin = {"batch": batch, "items": twin}
    to_other = {"batch": other, "items": index}
    to_diag = {"batch": other, "items": twin}

    def remote(src, dst, ss, rs, device):
        return pltpu.make_async_remote_copy(
            src_ref=src, dst_ref=dst, send_sem=ss, recv_sem=rs, device_id=device, device_id_type=MESH
        )

    barrier = pltpu.get_barrier_semaphore()

    def steps(count, first, body):
        if count <= 8:
            for step in range(count - 1, first - 1, -1):
                body(step)
        else:
            pl.loop(first, count)(body)

    def each(body):
        steps(peers, 1, body)

    def rising(body):
        if peers <= 8:
            for step in range(1, peers):
                body(step)
        else:
            pl.loop(1, peers)(body)

    def low_first(body):
        if peers <= 8:
            for peer in range(peers):
                body(peer)
        else:
            pl.loop(0, peers)(body)

    def greet(step):
        peer = peer_at(step)

        @pl.when(peer > me)
        def _():
            pl.semaphore_signal(barrier, inc=1, device_id=at(peer), device_id_type=MESH)

    def answer(peer):
        @pl.when(peer < me)
        def _():
            pl.semaphore_signal(ready.at[me], inc=1, device_id=at(peer), device_id_type=MESH)

    mine_in = (
        pltpu.make_async_copy(items_ref, iall.at[0], in_sem.at[0]),
        pltpu.make_async_copy(users_ref, uall.at[me], in_sem.at[1]),
        pltpu.make_async_copy(pos_ref, pall.at[me], in_sem.at[2]),
    )
    each(greet)
    pl.semaphore_signal(barrier, inc=1, device_id=to_twin, device_id_type=MESH)

    @pl.when(batch == 0)
    def _():
        pl.semaphore_signal(barrier, inc=1, device_id=to_other, device_id_type=MESH)

    for copy in mine_in:
        copy.start()
    pl.semaphore_wait(barrier, me + batch + 1)
    @pl.when(batch == 1)
    def _():
        pl.semaphore_signal(x_ready.at[0], inc=1, device_id=to_other, device_id_type=MESH)

    low_first(answer)

    for copy in mine_in:
        copy.wait()

    def users_copy(step, source):
        return remote(uall.at[me], uall.at[source], u_ss.at[step], u_rs.at[source], at(peer_at(step)))

    def pos_copy(step, source):
        return remote(pall.at[me], pall.at[source], p_ss.at[step], p_rs.at[source], at(peer_at(step)))

    def stat_copy(step, source):
        return remote(stat, stat_all.at[source], s_ss.at[step], s_rs.at[source], at(peer_at(step)))

    half = peers // 2
    side = me // half
    place = lax.rem(me, half)

    def near_at(step):
        return side * half + lax.rem(place + step, half)

    def far_at(step):
        return (1 - side) * half + lax.rem(place + step, half)

    def near_copy(step, source):
        return to_near(near_at(step), source)

    def far_copy(step, source):
        return to_far(far_at(step), source)

    def to_near(peer, source):
        return remote(term.at[peer], near_recv.at[source], g_ss.at[peer], g_rs.at[source], at(peer))

    def to_far(peer, source):
        return remote(ug_send.at[peer], far_recv.at[source], g_ss.at[peer], g_rs.at[source], at(peer))

    half_rows = per // PARTS

    def items_copy(source, slot, p, device):
        block = pl.ds(p * half_rows, half_rows)
        return remote(
            iall.at[source, block], iall.at[slot, block], i_ss.at[slot, p], i_rs.at[slot, p], device
        )

    from_other = [items_copy(0, 2, p, to_other) for p in range(PARTS)]
    from_twin = [items_copy(0, 1, p, to_twin) for p in range(PARTS)]
    from_diag = [items_copy(2, 3, p, to_twin) for p in range(PARTS)]

    def send_down(peer):
        step = lax.rem(peer - me + peers, peers)

        @pl.when(peer < me)
        def _():
            users_copy(step, me).start()
            pos_copy(step, me).start()

    def send_up(step):
        peer = peer_at(step)

        @pl.when(peer > me)
        def _():
            pl.semaphore_wait(ready.at[peer], 1)
            users_copy(step, me).start()
            pos_copy(step, me).start()

    @pl.when(batch == 1)
    def _():
        for copy in from_other:
            copy.start()

    low_first(send_down)
    for copy in from_twin:
        copy.start()

    @pl.when(batch == 0)
    def _():
        pl.semaphore_wait(x_ready.at[0], 1)
        for copy in from_other:
            copy.start()

    rising(send_up)
    for p in range(PARTS):
        from_other[p].wait_recv()
        from_diag[p].start()
    def near_in(step):
        source = near_at(step)
        users_copy(step, source).wait_recv()

    def far_in(step):
        source = far_at(step)
        users_copy(step, source).wait_recv()

    def mate_copy(src, k, p, part, device):
        block = pl.ds(part * half, half)
        return remote(src.at[block], mates.at[k, block], m_ss.at[k, p], m_rs.at[k, p], device)

    def ids_copy(src, k, device):
        return remote(src, mate_ids.at[k], n_ss.at[k], n_rs.at[k], device)

    ids_to_mates = (ids_copy(pall, 1, to_other), ids_copy(pall, 0, to_twin))
    ids_onward = ids_copy(mate_ids.at[1], 2, to_twin)

    halves = (side, 1 - side)
    to_mates = [
        [mate_copy(uall, 1, p, halves[p], to_other) for p in range(2)],
        [mate_copy(uall, 0, p, halves[p], to_twin) for p in range(2)],
    ]
    onward = [mate_copy(mates.at[1], 2, p, halves[p], to_twin) for p in range(2)]

    def lend(p):
        for pair in to_mates:
            pair[p].start()

    steps(half, 1, near_in)
    lend(0)

    def over_chunks(body):
        if chunks <= 2:
            for chunk in range(chunks):
                body(chunk)
        else:
            pl.loop(0, chunks)(body)

    def over_half(which, body):
        count = chunks // 2
        if count == 1:
            body(which)
        else:
            pl.loop(0, count)(lambda chunk: body(which * count + chunk))

    homes = (
        batch * total_index + index,
        batch * total_index + twin,
        other * total_index + index,
        other * total_index + twin,
    )
    row = lax.broadcasted_iota(jnp.int32, (per, slots * own), 0)

    def lane_ids(ids, chunk):
        return jnp.concatenate([ids[chunk * slots + k] for k in range(slots)], axis=1)

    def ids_of(chunk):
        return lane_ids(pall, chunk)

    def joined(blocks, chunk):
        return jnp.concatenate(
            [blocks[chunk * slots + k].astype(F32) for k in range(slots)], axis=0
        ).astype(BF16)

    def prepare(chunk):
        ucat[chunk] = joined(uall, chunk)

    def meet(k, chunk):
        mate_cat[k, chunk] = joined(mates.at[k], chunk)
        mate_logit[k, chunk] = lax.dot_general(
            iall[0], mate_cat[k, chunk], NT, preferred_element_type=F32
        )

    def folded(combine, block):
        return combine(block.reshape(block.shape[0] // 8, 8, block.shape[1]), axis=0)

    def forward(chunk):
        logits = [
            lax.dot_general(iall[q], ucat[chunk], NT, preferred_element_type=F32)
            for q in range(QUAD)
        ]
        tops = [folded(jnp.max, logit) for logit in logits]
        top = jnp.max(functools.reduce(jnp.maximum, tops), axis=0, keepdims=True)
        total = jnp.zeros_like(tops[0])
        for q in range(QUAD):
            e = jnp.exp(logits[q] - top)
            e_ref[chunk, q * per : (q + 1) * per] = e.astype(BF16)
            total = total + folded(jnp.sum, e)
        stat[chunk] = top + jnp.log(jnp.sum(total, axis=0, keepdims=True))
        top_ref[chunk] = top
        logit_ref[chunk] = logits[0]

    for copy in from_twin + from_diag:
        copy.wait_recv()

    def advance(chunk):
        prepare(chunk)
        forward(chunk)

    over_half(side, advance)
    steps(half, 0, far_in)
    over_half(1 - side, advance)
    def tell(peer):
        @pl.when(peer != me)
        def _():
            stat_copy(lax.rem(peer - me + peers, peers), me).start()

    low_first(tell)
    stat_all[me] = stat[...]
    lend(1)
    each(lambda step: pos_copy(step, peer_at(step)).wait_recv())
    for copy in ids_to_mates:
        copy.start()

    def mate_in(k, p):
        mate_copy(uall, k, p, halves[p], to_twin).wait_recv()

    def columns(rows):
        return jnp.transpose(jnp.concatenate([rows] * (8 // rows.shape[0]), axis=0))

    def gather_terms(chunk):
        mix = jnp.zeros((slots * own, ucat.shape[2]), F32)
        pick = jnp.zeros((slots * own, ucat.shape[2]), F32)
        for q in range(QUAD):
            here = row == ids_of(chunk) - homes[q] * per
            hit = jnp.where(here, 1.0, 0.0).astype(BF16)
            rest = jnp.where(here, 0.0, e_ref[chunk, q * per : (q + 1) * per].astype(F32)).astype(BF16)
            part = lax.dot_general(rest, iall[q], TN, preferred_element_type=F32)
            mix = mix + part
            pick = pick + lax.dot_general(hit, iall[q], TN, preferred_element_type=F32)
        blend[chunk] = mix
        picked[chunk] = pick
        pos[chunk] = lax.dot_general(
            jnp.ones((8, pick.shape[1]), F32), ucat[chunk].astype(F32) * pick, NT,
            precision=lax.Precision.HIGHEST, preferred_element_type=F32,
        )[0:1]

    def pos_out(step, source):
        return remote(pos, pos_all.at[source], h_ss.at[step], h_rs.at[source], at(peer_at(step)))

    over_chunks(gather_terms)
    each(lambda step: pos_out(step, me).start())
    pos_all[me] = pos[...]
    for p in range(2):
        mate_in(0, p)
    over_chunks(functools.partial(meet, 0))
    mate_in(1, 0)
    onward[0].start()
    for copy in from_other + from_twin + from_diag:
        copy.wait_send()
    for copy in (users_copy, pos_copy):
        each(lambda step: copy(step, me).wait_send())
    each(lambda step: stat_copy(step, peer_at(step)).wait_recv())


    def rescale(chunk):
        lses = stat_all[:, chunk]
        peak = jnp.max(lses, axis=0)
        lse_ref[chunk] = peak + jnp.log(jnp.sum(jnp.exp(lses - peak[None]), axis=0))

    def user_terms(chunk):
        lse = lse_ref[chunk]
        at_pos = jnp.exp(jnp.minimum(pos[chunk] - lse, 0.0)) - 1.0
        at_top = jnp.exp(top_ref[chunk] - lse)
        scale = columns(jnp.concatenate([at_top, at_pos], axis=0).astype(BF16).astype(F32))
        grad = blend[chunk] * scale[:, 0:1] + picked[chunk] * scale[:, 1:2]
        for k in range(slots):
            part = grad[k * own : (k + 1) * own]
            term[chunk * slots + k] = part
            ug_send[chunk * slots + k] = part.astype(BF16)

    def own_term(chunk):
        hit = row == ids_of(chunk) - homes[0] * per
        w = jnp.exp(logit_ref[chunk] - lse_ref[chunk]) - jnp.where(hit, 1.0, 0.0)
        return jnp.dot(w.astype(BF16), ucat[chunk], preferred_element_type=F32)

    def mate_term(k, chunk):
        hit = row == lane_ids(mate_ids.at[k], chunk) - homes[0] * per
        w = jnp.exp(mate_logit[k, chunk] - mate_lse[k, chunk]) - jnp.where(hit, 1.0, 0.0)
        return jnp.dot(w.astype(BF16), mate_cat[k, chunk], preferred_element_type=F32)

    def total_of(one):
        if chunks == 2:
            return one(0) + one(1)
        return lax.fori_loop(1, chunks, lambda chunk, acc: acc + one(chunk), one(0))

    lse_copies = [
        remote(lse_ref, mate_lse.at[k], l_ss.at[k], l_rs.at[k], device)
        for k, device in enumerate((to_twin, to_other, to_diag))
    ]

    def give(peer):
        @pl.when(peer // half != side)
        def _():
            to_far(peer, me).start()

        @pl.when(jnp.logical_and(peer // half == side, peer != me))
        def _():
            to_near(peer, me).start()

    def send_terms(chunk):
        user_terms(chunk)
        if chunks <= 2:
            for k in range(slots):
                give(chunk * slots + k)
        else:
            pl.loop(0, slots)(lambda k: give(chunk * slots + k))

    def send_lses():
        for copy in (lse_copies[1], lse_copies[2], lse_copies[0]):
            copy.start()

    if chunks <= 2:
        rescale(0)
        send_terms(0)
        for chunk in range(1, chunks):
            rescale(chunk)
        send_lses()
        for chunk in range(1, chunks):
            send_terms(chunk)
    else:
        over_chunks(rescale)
        send_lses()
        over_chunks(send_terms)
    ig_ref[...] = total_of(own_term)
    mate_in(1, 1)
    onward[1].start()
    ids_to_mates[0].wait_recv()
    ids_onward.start()
    over_chunks(functools.partial(meet, 1))
    for p in range(2):
        mate_in(2, p)
    over_chunks(functools.partial(meet, 2))
    each(lambda step: stat_copy(step, me).wait_send())
    each(lambda step: pos_out(step, me).wait_send())
    for p in range(2):
        for copy in (to_mates[0][p], to_mates[1][p], onward[p]):
            copy.wait_send()
    for copy in (*ids_to_mates, ids_onward):
        copy.wait_send()
    ids_to_mates[1].wait_recv()
    ids_onward.wait_recv()
    for copy in lse_copies:
        copy.wait_send()
    for k in (0, 2, 1):
        lse_copies[k].wait_recv()
        ig_ref[...] += total_of(functools.partial(mate_term, k))

    each(lambda step: pos_out(step, peer_at(step)).wait_recv())
    losses = lse_ref[me // slots] - jnp.sum(pos_all[:, me // slots], axis=0)
    loss = jnp.zeros((1, own), F32)
    for k in range(slots):
        loss = jnp.where(lax.rem(me, slots) == k, losses[:, k * own : (k + 1) * own], loss)
    loss_ref[...] = loss

    ug_ref[...] = term[me]

    def gather_near(step):
        near_copy(step, near_at(step)).wait_recv()
        ug_ref[...] += near_recv[near_at(step)]

    def gather_far(step):
        far_copy(step, far_at(step)).wait_recv()
        ug_ref[...] += far_recv[far_at(step)].astype(F32)

    steps(half, 0, lambda step: far_copy(step, me).wait_send())
    steps(half, 1, lambda step: near_copy(step, me).wait_send())
    steps(half, 1, gather_near)
    steps(half, 0, gather_far)


def settle(loss_in, ug_in, ig_in, loss_out, ug_out, ig_out, sems):
    copies = [
        pltpu.make_async_copy(src, dst, sems.at[k])
        for k, (src, dst) in enumerate(((ig_in, ig_out), (ug_in, ug_out), (loss_in, loss_out)))
    ]
    for copy in copies:
        copy.start()
    for copy in copies:
        copy.wait()


def local(users, items, pos_ids):
    own, width = users.shape
    per = items.shape[0]
    peers = lax.axis_size("items") // 2
    slots = math.gcd(peers // 2, 4)
    chunks = peers // slots
    lanes = slots * own
    dma = pltpu.SemaphoreType.DMA
    vmem = pl.BlockSpec(memory_space=pltpu.VMEM)
    hbm = pl.BlockSpec(memory_space=pltpu.HBM)
    loss, user_grad, item_grad = pl.pallas_call(
        functools.partial(kernel, peers, slots),
        out_shape=(
            pltpu.VMEM((1, own), F32),
            pltpu.VMEM((own, width), F32),
            pltpu.VMEM((per, width), F32),
        ),
        in_specs=[hbm] * 3,
        out_specs=(vmem, vmem, vmem),
        scratch_shapes=[
            pltpu.VMEM((peers, own, width), BF16),
            pltpu.VMEM((peers, 1, own), jnp.int32),
            pltpu.VMEM((QUAD, per, width), BF16),
            pltpu.VMEM((chunks, lanes, width), BF16),
            pltpu.VMEM((chunks, QUAD * per, lanes), BF16),
            pltpu.VMEM((chunks, per, lanes), F32),
            pltpu.VMEM((chunks, lanes, width), F32),
            pltpu.VMEM((chunks, lanes, width), F32),
            pltpu.VMEM((chunks, 1, lanes), F32),
            pltpu.VMEM((chunks, 1, lanes), F32),
            pltpu.VMEM((peers, chunks, 1, lanes), F32),
            pltpu.VMEM((chunks, 1, lanes), F32),
            pltpu.VMEM((peers, chunks, 1, lanes), F32),
            pltpu.VMEM((peers, own, width), F32),
            pltpu.VMEM((peers, own, width), BF16),
            pltpu.VMEM((peers, own, width), F32),
            pltpu.VMEM((peers, own, width), BF16),
            pltpu.VMEM((3, peers, own, width), BF16),
            pltpu.VMEM((3, peers, 1, own), jnp.int32),
            pltpu.VMEM((3, chunks, lanes, width), BF16),
            pltpu.VMEM((3, chunks, per, lanes), F32),
            pltpu.VMEM((chunks, 1, lanes), F32),
            pltpu.VMEM((3, chunks, 1, lanes), F32),
            dma((peers,)), dma((peers,)),
            dma((peers,)), dma((peers,)),
            dma((QUAD, PARTS)), dma((QUAD, PARTS)),
            dma((peers,)), dma((peers,)),
            dma((peers,)), dma((peers,)),
            dma((peers,)), dma((peers,)),
            dma((3, 2)), dma((3, 2)),
            dma((3,)), dma((3,)),
            dma((3,)), dma((3,)),
            dma((3,)),
            pltpu.SemaphoreType.REGULAR((peers,)),
            pltpu.SemaphoreType.REGULAR((1,)),
        ],
        compiler_params=pltpu.CompilerParams(
            collective_id=0, has_side_effects=True, vmem_limit_bytes=56 * 1024 * 1024
        ),
    )(*(pltpu.with_memory_space_constraint(v, pltpu.HBM) for v in (users, items, pos_ids.reshape(1, own))))
    loss, user_grad, item_grad = pl.pallas_call(
        settle,
        out_shape=(
            jax.ShapeDtypeStruct((1, own), F32),
            jax.ShapeDtypeStruct((own, width), F32),
            jax.ShapeDtypeStruct((per, width), F32),
        ),
        in_specs=[vmem] * 3,
        out_specs=(hbm,) * 3,
        scratch_shapes=[dma((3,))],
        compiler_params=pltpu.CompilerParams(vmem_limit_bytes=4 * 1024 * 1024),
    )(loss, user_grad, item_grad)
    return loss.reshape(own), user_grad, item_grad


def solution(mesh):
    placed = (P(("batch", "items"), None), P(("batch", "items"), None), P(("batch", "items")))
    return jax.shard_map(
        local,
        mesh=mesh,
        in_specs=placed,
        out_specs=(P(("batch", "items")), P(("batch", "items"), None), P(("batch", "items"), None)),
        check_vma=False,
    )
```

```python
import functools
import math

import jax
import jax.numpy as jnp
from jax import lax
from jax.experimental import pallas as pl
from jax.experimental.pallas import tpu as pltpu
from jax.sharding import PartitionSpec as P

F32 = jnp.float32
BF16 = jnp.bfloat16
MESH = pl.DeviceIdType.MESH
NT = (((1,), (1,)), ((), ()))
TN = (((0,), (0,)), ((), ()))
QUAD = 4
PARTS = 1


def kernel(
    peers, slots, users_ref, items_ref, pos_ref,
    loss_ref, ug_ref, ig_ref,
    uall, pall, iall, ucat, e_ref, logit_ref, blend, picked, top_ref, stat, stat_all, pos, pos_all,
    term, ug_send, near_recv, far_recv, mates, mate_ids, mate_cat, mate_logit, lse_ref, mate_lse,
    u_ss, u_rs, p_ss, p_rs, i_ss, i_rs, s_ss, s_rs, h_ss, h_rs, g_ss, g_rs, m_ss, m_rs, n_ss, n_rs, l_ss, l_rs,
    in_sem, ready, x_ready,
):
    own = users_ref.shape[0]
    per = items_ref.shape[0]
    chunks = peers // slots
    batch = lax.axis_index("batch")
    index = lax.axis_index("items")
    core = lax.rem(index, 2)
    me = index // 2
    twin = index + 1 - 2 * core
    other = 1 - batch
    total_index = 2 * peers

    def at(peer):
        return {"batch": batch, "items": 2 * peer + core}

    def peer_at(step):
        return lax.rem(me + step, peers)

    to_twin = {"batch": batch, "items": twin}
    to_other = {"batch": other, "items": index}
    to_diag = {"batch": other, "items": twin}

    def remote(src, dst, ss, rs, device):
        return pltpu.make_async_remote_copy(
            src_ref=src, dst_ref=dst, send_sem=ss, recv_sem=rs, device_id=device, device_id_type=MESH
        )

    barrier = pltpu.get_barrier_semaphore()

    def steps(count, first, body):
        if count <= 8:
            for step in range(count - 1, first - 1, -1):
                body(step)
        else:
            pl.loop(first, count)(body)

    def each(body):
        steps(peers, 1, body)

    def rising(body):
        if peers <= 8:
            for step in range(1, peers):
                body(step)
        else:
            pl.loop(1, peers)(body)

    def low_first(body):
        if peers <= 8:
            for peer in range(peers):
                body(peer)
        else:
            pl.loop(0, peers)(body)

    def greet(step):
        peer = peer_at(step)

        @pl.when(peer > me)
        def _():
            pl.semaphore_signal(barrier, inc=1, device_id=at(peer), device_id_type=MESH)

    def answer(peer):
        @pl.when(peer < me)
        def _():
            pl.semaphore_signal(ready.at[me], inc=1, device_id=at(peer), device_id_type=MESH)

    mine_in = (
        pltpu.make_async_copy(items_ref, iall.at[0], in_sem.at[0]),
        pltpu.make_async_copy(users_ref, uall.at[me], in_sem.at[1]),
        pltpu.make_async_copy(pos_ref, pall.at[me], in_sem.at[2]),
    )
    each(greet)
    pl.semaphore_signal(barrier, inc=1, device_id=to_twin, device_id_type=MESH)

    @pl.when(batch == 0)
    def _():
        pl.semaphore_signal(barrier, inc=1, device_id=to_other, device_id_type=MESH)

    for copy in mine_in:
        copy.start()
    pl.semaphore_wait(barrier, me + batch + 1)
    @pl.when(batch == 1)
    def _():
        pl.semaphore_signal(x_ready.at[0], inc=1, device_id=to_other, device_id_type=MESH)

    low_first(answer)

    for copy in mine_in:
        copy.wait()

    def users_copy(step, source):
        return remote(uall.at[me], uall.at[source], u_ss.at[step], u_rs.at[source], at(peer_at(step)))

    def pos_copy(step, source):
        return remote(pall.at[me], pall.at[source], p_ss.at[step], p_rs.at[source], at(peer_at(step)))

    def stat_copy(step, source):
        return remote(stat, stat_all.at[source], s_ss.at[step], s_rs.at[source], at(peer_at(step)))

    half = peers // 2
    side = me // half
    place = lax.rem(me, half)

    def near_at(step):
        return side * half + lax.rem(place + step, half)

    def far_at(step):
        return (1 - side) * half + lax.rem(place + step, half)

    def near_copy(step, source):
        return to_near(near_at(step), source)

    def far_copy(step, source):
        return to_far(far_at(step), source)

    def to_near(peer, source):
        return remote(term.at[peer], near_recv.at[source], g_ss.at[peer], g_rs.at[source], at(peer))

    def to_far(peer, source):
        return remote(ug_send.at[peer], far_recv.at[source], g_ss.at[peer], g_rs.at[source], at(peer))

    half_rows = per // PARTS

    def items_copy(source, slot, p, device):
        block = pl.ds(p * half_rows, half_rows)
        return remote(
            iall.at[source, block], iall.at[slot, block], i_ss.at[slot, p], i_rs.at[slot, p], device
        )

    from_other = [items_copy(0, 2, p, to_other) for p in range(PARTS)]
    from_twin = [items_copy(0, 1, p, to_twin) for p in range(PARTS)]
    from_diag = [items_copy(2, 3, p, to_twin) for p in range(PARTS)]

    def send_down(peer):
        step = lax.rem(peer - me + peers, peers)

        @pl.when(peer < me)
        def _():
            users_copy(step, me).start()
            pos_copy(step, me).start()

    def send_up(step):
        peer = peer_at(step)

        @pl.when(peer > me)
        def _():
            pl.semaphore_wait(ready.at[peer], 1)
            users_copy(step, me).start()
            pos_copy(step, me).start()

    @pl.when(batch == 1)
    def _():
        for copy in from_other:
            copy.start()

    low_first(send_down)
    for copy in from_twin:
        copy.start()

    @pl.when(batch == 0)
    def _():
        pl.semaphore_wait(x_ready.at[0], 1)
        for copy in from_other:
            copy.start()

    rising(send_up)
    for p in range(PARTS):
        from_other[p].wait_recv()
        from_diag[p].start()
    def near_in(step):
        source = near_at(step)
        users_copy(step, source).wait_recv()

    def far_in(step):
        source = far_at(step)
        users_copy(step, source).wait_recv()

    def mate_copy(src, k, p, part, device):
        block = pl.ds(part * half, half)
        return remote(src.at[block], mates.at[k, block], m_ss.at[k, p], m_rs.at[k, p], device)

    def ids_copy(src, k, device):
        return remote(src, mate_ids.at[k], n_ss.at[k], n_rs.at[k], device)

    ids_to_mates = (ids_copy(pall, 1, to_other), ids_copy(pall, 0, to_twin))
    ids_onward = ids_copy(mate_ids.at[1], 2, to_twin)

    halves = (side, 1 - side)
    to_mates = [
        [mate_copy(uall, 1, p, halves[p], to_other) for p in range(2)],
        [mate_copy(uall, 0, p, halves[p], to_twin) for p in range(2)],
    ]
    onward = [mate_copy(mates.at[1], 2, p, halves[p], to_twin) for p in range(2)]

    def lend(p):
        for pair in to_mates:
            pair[p].start()

    steps(half, 1, near_in)
    lend(0)

    def over_chunks(body):
        if chunks <= 2:
            for chunk in range(chunks):
                body(chunk)
        else:
            pl.loop(0, chunks)(body)

    def over_half(which, body):
        count = chunks // 2
        if count == 1:
            body(which)
        else:
            pl.loop(0, count)(lambda chunk: body(which * count + chunk))

    homes = (
        batch * total_index + index,
        batch * total_index + twin,
        other * total_index + index,
        other * total_index + twin,
    )
    row = lax.broadcasted_iota(jnp.int32, (per, slots * own), 0)

    def lane_ids(ids, chunk):
        return jnp.concatenate([ids[chunk * slots + k] for k in range(slots)], axis=1)

    def ids_of(chunk):
        return lane_ids(pall, chunk)

    def joined(blocks, chunk):
        return jnp.concatenate(
            [blocks[chunk * slots + k].astype(F32) for k in range(slots)], axis=0
        ).astype(BF16)

    def prepare(chunk):
        ucat[chunk] = joined(uall, chunk)

    def meet(k, chunk):
        mate_cat[k, chunk] = joined(mates.at[k], chunk)
        mate_logit[k, chunk] = lax.dot_general(
            iall[0], mate_cat[k, chunk], NT, preferred_element_type=F32
        )

    def folded(combine, block):
        return combine(block.reshape(block.shape[0] // 8, 8, block.shape[1]), axis=0)

    def forward(chunk):
        logits = [
            lax.dot_general(iall[q], ucat[chunk], NT, preferred_element_type=F32)
            for q in range(QUAD)
        ]
        tops = [folded(jnp.max, logit) for logit in logits]
        top = jnp.max(functools.reduce(jnp.maximum, tops), axis=0, keepdims=True)
        total = jnp.zeros_like(tops[0])
        for q in range(QUAD):
            e = jnp.exp(logits[q] - top)
            e_ref[chunk, q * per : (q + 1) * per] = e.astype(BF16)
            total = total + folded(jnp.sum, e)
        stat[chunk] = top + jnp.log(jnp.sum(total, axis=0, keepdims=True))
        top_ref[chunk] = top
        logit_ref[chunk] = logits[0]

    for copy in from_twin + from_diag:
        copy.wait_recv()

    def advance(chunk):
        prepare(chunk)
        forward(chunk)

    over_half(side, advance)
    steps(half, 0, far_in)
    over_half(1 - side, advance)
    def tell(peer):
        @pl.when(peer != me)
        def _():
            stat_copy(lax.rem(peer - me + peers, peers), me).start()

    low_first(tell)
    stat_all[me] = stat[...]
    lend(1)
    each(lambda step: pos_copy(step, peer_at(step)).wait_recv())
    for copy in ids_to_mates:
        copy.start()

    def mate_in(k, p):
        mate_copy(uall, k, p, halves[p], to_twin).wait_recv()

    def columns(rows):
        return jnp.transpose(jnp.concatenate([rows] * (8 // rows.shape[0]), axis=0))

    def gather_terms(chunk):
        mix = jnp.zeros((slots * own, ucat.shape[2]), F32)
        pick = jnp.zeros((slots * own, ucat.shape[2]), F32)
        for q in range(QUAD):
            here = row == ids_of(chunk) - homes[q] * per
            hit = jnp.where(here, 1.0, 0.0).astype(BF16)
            rest = jnp.where(here, 0.0, e_ref[chunk, q * per : (q + 1) * per].astype(F32)).astype(BF16)
            part = lax.dot_general(rest, iall[q], TN, preferred_element_type=F32)
            mix = mix + part
            pick = pick + lax.dot_general(hit, iall[q], TN, preferred_element_type=F32)
        blend[chunk] = mix
        picked[chunk] = pick
        pos[chunk] = lax.dot_general(
            jnp.ones((8, pick.shape[1]), F32), ucat[chunk].astype(F32) * pick, NT,
            precision=lax.Precision.HIGHEST, preferred_element_type=F32,
        )[0:1]

    def pos_out(step, source):
        return remote(pos, pos_all.at[source], h_ss.at[step], h_rs.at[source], at(peer_at(step)))

    over_chunks(gather_terms)
    each(lambda step: pos_out(step, me).start())
    pos_all[me] = pos[...]
    for p in range(2):
        mate_in(0, p)
    over_chunks(functools.partial(meet, 0))
    mate_in(1, 0)
    onward[0].start()
    for copy in from_other + from_twin + from_diag:
        copy.wait_send()
    for copy in (users_copy, pos_copy):
        each(lambda step: copy(step, me).wait_send())
    each(lambda step: stat_copy(step, peer_at(step)).wait_recv())


    def rescale(chunk):
        lses = stat_all[:, chunk]
        peak = jnp.max(lses, axis=0)
        lse_ref[chunk] = peak + jnp.log(jnp.sum(jnp.exp(lses - peak[None]), axis=0))

    def user_terms(chunk):
        lse = lse_ref[chunk]
        at_pos = jnp.exp(jnp.minimum(pos[chunk] - lse, 0.0)) - 1.0
        at_top = jnp.exp(top_ref[chunk] - lse)
        scale = columns(jnp.concatenate([at_top, at_pos], axis=0).astype(BF16).astype(F32))
        grad = blend[chunk] * scale[:, 0:1] + picked[chunk] * scale[:, 1:2]
        for k in range(slots):
            part = grad[k * own : (k + 1) * own]
            term[chunk * slots + k] = part
            ug_send[chunk * slots + k] = part.astype(BF16)

    def own_term(chunk):
        hit = row == ids_of(chunk) - homes[0] * per
        w = jnp.exp(logit_ref[chunk] - lse_ref[chunk]) - jnp.where(hit, 1.0, 0.0)
        return jnp.dot(w.astype(BF16), ucat[chunk], preferred_element_type=F32)

    def mate_term(k, chunk):
        hit = row == lane_ids(mate_ids.at[k], chunk) - homes[0] * per
        w = jnp.exp(mate_logit[k, chunk] - mate_lse[k, chunk]) - jnp.where(hit, 1.0, 0.0)
        return jnp.dot(w.astype(BF16), mate_cat[k, chunk], preferred_element_type=F32)

    def total_of(one):
        if chunks == 2:
            return one(0) + one(1)
        return lax.fori_loop(1, chunks, lambda chunk, acc: acc + one(chunk), one(0))

    lse_copies = [
        remote(lse_ref, mate_lse.at[k], l_ss.at[k], l_rs.at[k], device)
        for k, device in enumerate((to_twin, to_other, to_diag))
    ]

    def give(peer):
        @pl.when(peer // half != side)
        def _():
            to_far(peer, me).start()

        @pl.when(jnp.logical_and(peer // half == side, peer != me))
        def _():
            to_near(peer, me).start()

    def send_terms(chunk):
        user_terms(chunk)
        if chunks <= 2:
            for k in range(slots):
                give(chunk * slots + k)
        else:
            pl.loop(0, slots)(lambda k: give(chunk * slots + k))

    def send_lses():
        for copy in (lse_copies[1], lse_copies[2], lse_copies[0]):
            copy.start()

    if chunks <= 2:
        rescale(0)
        send_terms(0)
        for chunk in range(1, chunks):
            rescale(chunk)
        send_lses()
        for chunk in range(1, chunks):
            send_terms(chunk)
    else:
        over_chunks(rescale)
        send_lses()
        over_chunks(send_terms)
    ig_ref[...] = total_of(own_term)
    mate_in(1, 1)
    onward[1].start()
    ids_to_mates[0].wait_recv()
    ids_onward.start()
    over_chunks(functools.partial(meet, 1))
    for p in range(2):
        mate_in(2, p)
    over_chunks(functools.partial(meet, 2))
    each(lambda step: stat_copy(step, me).wait_send())
    each(lambda step: pos_out(step, me).wait_send())
    for p in range(2):
        for copy in (to_mates[0][p], to_mates[1][p], onward[p]):
            copy.wait_send()
    for copy in (*ids_to_mates, ids_onward):
        copy.wait_send()
    ids_to_mates[1].wait_recv()
    ids_onward.wait_recv()
    for copy in lse_copies:
        copy.wait_send()
    for k in (0, 2, 1):
        lse_copies[k].wait_recv()
        ig_ref[...] += total_of(functools.partial(mate_term, k))

    each(lambda step: pos_out(step, peer_at(step)).wait_recv())
    losses = lse_ref[me // slots] - jnp.sum(pos_all[:, me // slots], axis=0)
    loss = jnp.zeros((1, own), F32)
    for k in range(slots):
        loss = jnp.where(lax.rem(me, slots) == k, losses[:, k * own : (k + 1) * own], loss)
    loss_ref[...] = loss

    ug_ref[...] = term[me]

    def gather_near(step):
        near_copy(step, near_at(step)).wait_recv()
        ug_ref[...] += near_recv[near_at(step)]

    def gather_far(step):
        far_copy(step, far_at(step)).wait_recv()
        ug_ref[...] += far_recv[far_at(step)].astype(F32)

    steps(half, 0, lambda step: far_copy(step, me).wait_send())
    steps(half, 1, lambda step: near_copy(step, me).wait_send())
    steps(half, 1, gather_near)
    steps(half, 0, gather_far)


def settle(loss_in, ug_in, ig_in, loss_out, ug_out, ig_out, sems):
    copies = [
        pltpu.make_async_copy(src, dst, sems.at[k])
        for k, (src, dst) in enumerate(((ig_in, ig_out), (ug_in, ug_out), (loss_in, loss_out)))
    ]
    for copy in copies:
        copy.start()
    for copy in copies:
        copy.wait()


def local(users, items, pos_ids):
    own, width = users.shape
    per = items.shape[0]
    peers = lax.axis_size("items") // 2
    slots = math.gcd(peers // 2, 4)
    chunks = peers // slots
    lanes = slots * own
    dma = pltpu.SemaphoreType.DMA
    vmem = pl.BlockSpec(memory_space=pltpu.VMEM)
    hbm = pl.BlockSpec(memory_space=pltpu.HBM)
    loss, user_grad, item_grad = pl.pallas_call(
        functools.partial(kernel, peers, slots),
        out_shape=(
            pltpu.VMEM((1, own), F32),
            pltpu.VMEM((own, width), F32),
            pltpu.VMEM((per, width), F32),
        ),
        in_specs=[hbm] * 3,
        out_specs=(vmem, vmem, vmem),
        scratch_shapes=[
            pltpu.VMEM((peers, own, width), BF16),
            pltpu.VMEM((peers, 1, own), jnp.int32),
            pltpu.VMEM((QUAD, per, width), BF16),
            pltpu.VMEM((chunks, lanes, width), BF16),
            pltpu.VMEM((chunks, QUAD * per, lanes), BF16),
            pltpu.VMEM((chunks, per, lanes), F32),
            pltpu.VMEM((chunks, lanes, width), F32),
            pltpu.VMEM((chunks, lanes, width), F32),
            pltpu.VMEM((chunks, 1, lanes), F32),
            pltpu.VMEM((chunks, 1, lanes), F32),
            pltpu.VMEM((peers, chunks, 1, lanes), F32),
            pltpu.VMEM((chunks, 1, lanes), F32),
            pltpu.VMEM((peers, chunks, 1, lanes), F32),
            pltpu.VMEM((peers, own, width), F32),
            pltpu.VMEM((peers, own, width), BF16),
            pltpu.VMEM((peers, own, width), F32),
            pltpu.VMEM((peers, own, width), BF16),
            pltpu.VMEM((3, peers, own, width), BF16),
            pltpu.VMEM((3, peers, 1, own), jnp.int32),
            pltpu.VMEM((3, chunks, lanes, width), BF16),
            pltpu.VMEM((3, chunks, per, lanes), F32),
            pltpu.VMEM((chunks, 1, lanes), F32),
            pltpu.VMEM((3, chunks, 1, lanes), F32),
            dma((peers,)), dma((peers,)),
            dma((peers,)), dma((peers,)),
            dma((QUAD, PARTS)), dma((QUAD, PARTS)),
            dma((peers,)), dma((peers,)),
            dma((peers,)), dma((peers,)),
            dma((peers,)), dma((peers,)),
            dma((3, 2)), dma((3, 2)),
            dma((3,)), dma((3,)),
            dma((3,)), dma((3,)),
            dma((3,)),
            pltpu.SemaphoreType.REGULAR((peers,)),
            pltpu.SemaphoreType.REGULAR((1,)),
        ],
        compiler_params=pltpu.CompilerParams(
            collective_id=0, has_side_effects=True, vmem_limit_bytes=56 * 1024 * 1024
        ),
    )(*(pltpu.with_memory_space_constraint(v, pltpu.HBM) for v in (users, items, pos_ids.reshape(1, own))))
    loss, user_grad, item_grad = pl.pallas_call(
        settle,
        out_shape=(
            jax.ShapeDtypeStruct((1, own), F32),
            jax.ShapeDtypeStruct((own, width), F32),
            jax.ShapeDtypeStruct((per, width), F32),
        ),
        in_specs=[vmem] * 3,
        out_specs=(hbm,) * 3,
        scratch_shapes=[dma((3,))],
        compiler_params=pltpu.CompilerParams(vmem_limit_bytes=4 * 1024 * 1024),
    )(loss, user_grad, item_grad)
    return loss.reshape(own), user_grad, item_grad


def solution(mesh):
    placed = (P(("batch", "items"), None), P(("batch", "items"), None), P(("batch", "items")))
    return jax.shard_map(
        local,
        mesh=mesh,
        in_specs=placed,
        out_specs=(P(("batch", "items")), P(("batch", "items"), None), P(("batch", "items"), None)),
        check_vma=False,
    )
```
